32 devices in a mesh: blk: 8 (over y, x, core), chan: 4 (over z).
Axes of the slice: x: 2, y: 2, z: 4, core: 2. Of those that a mesh axis runs over, the one named last changes fastest.
Arguments:
- pair_repr: bfloat16 [512, 512, 128], P('blk', 'chan'), may hold values from -6 to 6
- chain_lengths: int32 [8], replicated, may hold values from 48 to 64
- norm_gain: float32 [128], replicated, may hold values from 0.1 to 1.9
- norm_bias: float32 [128], replicated, may hold values from -3 to 3
- left_gate: bfloat16 [128, 128], replicated, may hold values from -0.5 to 0.5
- left_value: bfloat16 [128, 128], replicated, may hold values from -0.5 to 0.5
- right_gate: bfloat16 [128, 128], replicated, may hold values from -0.5 to 0.5
- right_value: bfloat16 [128, 128], replicated, may hold values from -0.5 to 0.5
- out_gain: float32 [128], replicated, may hold values from 0.1 to 1.9
- out_bias: float32 [128], replicated, may hold values from -3 to 3
- out_weight: bfloat16 [128, 128], replicated, may hold values from -0.5 to 0.5
- gate_weight: bfloat16 [128, 128], replicated, may hold values from -0.5 to 0.5
Outputs:
- pair_update: bfloat16 [512, 104, 128], P('blk', 'chan')
The draws below stay inside these ranges and needn't reach their ends.
Inputs may be any that keep to these rules, and one draw needn't show every extreme that they name: Chain slot s covers residues s * 64 to (s + 1) * 64 - 1, of which the first chain_lengths[s] are real and the rest padding.
All inputs are finite; a program needn't handle non-finite values.
Results may differ from the reference program's by a relative error of at most 0.0058.
Values may be sent and summed in bfloat16 or wider, within the bound.
A program may use at most 64 MiB of HBM per device.

```python
import jax
import jax.numpy as jnp
from jax import lax

C = 128
CH = 128
ROWS_DEV = 64
JD = 13
NCHAIN = 8
NRES = 512
SLOT = 64
J = 104
N_BLK = 8


def place_ends(result, rng, smallest, largest):
    longest = result.shape.index(max(result.shape))
    spots = []
    for shift in (0, 1):
        where = [jax.random.randint(jax.random.fold_in(rng, axis), (), 0, length) for axis, length in enumerate(result.shape)]
        where[longest] = (where[longest] + shift) % result.shape[longest]
        spots.append(tuple(where))
    return result.at[spots[0]].set(smallest).at[spots[1]].set(largest)


def levels(key, shape, pieces, smallest, high):
    gain, own = 1.0, jax.random.fold_in(key, 6)
    for dim, shards_of in pieces:
        draws = jnp.exp(jax.random.uniform(jax.random.fold_in(own, dim), (shards_of,), jnp.float32, smallest / len(pieces), high / len(pieces)))
        gain = gain * jnp.repeat(draws, shape[dim] // shards_of).reshape([-1 if axis == dim else 1 for axis in range(len(shape))])
    return gain


def bell_draw(own_key, extent, scale, limit, split=(), held_as=jnp.bfloat16):
    result = scale * jax.random.normal(own_key, extent, jnp.float32)
    if split:
        result = result * levels(own_key, extent, split, -0.22, 0.18)
    return jnp.clip(result, -limit, limit).astype(held_as)


def setup_inputs(seed: int = 0) -> dict:
    arg_keys = jax.random.split(jax.random.key(seed), 13)
    pair_repr = bell_draw(arg_keys[0], (NRES, NRES, C), 1.0, 6.0, ((0, 8), (1, 4)))
    chain_lengths = place_ends(jax.random.randint(arg_keys[1], (NCHAIN,), 3 * SLOT // 4, SLOT + 1), jax.random.fold_in(arg_keys[1], 1), 3 * SLOT // 4, SLOT).astype(jnp.int32)
    norm_gain = jnp.clip(1.0 + 0.18 * jax.random.normal(arg_keys[2], (C,), jnp.float32), 0.1, 1.9)
    norm_bias = bell_draw(arg_keys[3], (C,), 0.5, 3.0, (), jnp.float32)
    left_gate = bell_draw(arg_keys[4], (C, CH), C ** -0.5, 0.5)
    left_value = bell_draw(arg_keys[5], (C, CH), C ** -0.5, 0.5)
    right_gate = bell_draw(arg_keys[6], (C, CH), C ** -0.5, 0.5)
    right_value = bell_draw(arg_keys[7], (C, CH), C ** -0.5, 0.5)
    out_gain = jnp.clip(1.0 + 0.18 * jax.random.normal(arg_keys[8], (CH,), jnp.float32), 0.1, 1.9)
    out_bias = bell_draw(arg_keys[9], (CH,), 0.5, 3.0, (), jnp.float32)
    out_weight = bell_draw(arg_keys[10], (CH, C), CH ** -0.5, 0.5)
    gate_weight = bell_draw(arg_keys[11], (C, C), C ** -0.5, 0.5)
    return dict(pair_repr=pair_repr, chain_lengths=chain_lengths, norm_gain=norm_gain, norm_bias=norm_bias, left_gate=left_gate, left_value=left_value, right_gate=right_gate, right_value=right_value, out_gain=out_gain, out_bias=out_bias, out_weight=out_weight, gate_weight=gate_weight)


epsilon = 1e-05

def normalize(values, gain_vec, bias_vec):
    centre = lax.optimization_barrier(jnp.mean(values, axis=-1, keepdims=True))
    centred = values - centre
    spread_sq = lax.optimization_barrier(jnp.mean(centred * centred, axis=-1, keepdims=True))
    return centred * lax.rsqrt(spread_sq + epsilon) * gain_vec + bias_vec

def residue_mask(position, lengths, slot_size):
    chain_id = position // slot_size
    chain_table = jnp.arange(lengths.shape[0], dtype=jnp.int32)
    chain_len = lax.optimization_barrier(jnp.sum(jnp.where(chain_id[:, None] == chain_table[None, :], lengths[None, :], 0), axis=1))
    return (position % slot_size < chain_len).astype(jnp.float32)

def reference(pair_repr, chain_lengths, norm_gain, norm_bias, left_gate, left_value, right_gate, right_value, out_gain, out_bias, out_weight, gate_weight):
    position = jnp.arange(NRES, dtype=jnp.int32)
    residue = residue_mask(position, chain_lengths, SLOT)
    window = (jnp.arange(N_BLK, dtype=jnp.int32)[:, None] * ROWS_DEV + jnp.arange(JD, dtype=jnp.int32)[None, :]).reshape(-1)
    window_normed = normalize(pair_repr[window].astype(jnp.float32), norm_gain, norm_bias).astype(jnp.bfloat16)
    window_flat = window_normed.reshape(-1, C)
    right_mix = jax.nn.sigmoid(jnp.dot(window_flat, right_gate, preferred_element_type=jnp.float32)) * jnp.dot(window_flat, right_value, preferred_element_type=jnp.float32)
    right_mix = right_mix.reshape(J, NRES, CH) * residue[window][:, None, None] * residue[None, :, None]
    right_wide = jnp.transpose(right_mix.astype(jnp.bfloat16).astype(jnp.float32), (2, 0, 1))

    def row_block(block_id):
        start_row = block_id * ROWS_DEV
        block_pair = lax.dynamic_slice_in_dim(pair_repr, start_row, ROWS_DEV, 0)
        normed = normalize(block_pair.astype(jnp.float32), norm_gain, norm_bias).astype(jnp.bfloat16)
        flat_rows = normed.reshape(-1, C)
        left_mix = jax.nn.sigmoid(jnp.dot(flat_rows, left_gate, preferred_element_type=jnp.float32)) * jnp.dot(flat_rows, left_value, preferred_element_type=jnp.float32)
        row_real = lax.dynamic_slice_in_dim(residue, start_row, ROWS_DEV, 0)
        left_mix = left_mix.reshape(ROWS_DEV, NRES, CH) * row_real[:, None, None] * residue[None, :, None]
        left_wide = jnp.transpose(left_mix.astype(jnp.bfloat16).astype(jnp.float32), (2, 0, 1))
        product = jnp.einsum('cik,cjk->cij', left_wide, right_wide).astype(jnp.bfloat16).astype(jnp.float32)
        centre = lax.optimization_barrier(jnp.mean(product, axis=0, keepdims=True))
        centred = product - centre
        spread_sq = lax.optimization_barrier(jnp.mean(centred * centred, axis=0, keepdims=True))
        normed_product = (centred * lax.rsqrt(spread_sq + epsilon) * out_gain[:, None, None] + out_bias[:, None, None]).astype(jnp.bfloat16)
        update = jnp.einsum('cij,cd->ijd', normed_product.astype(jnp.float32), out_weight.astype(jnp.float32))
        gate_rows = normed[:, window]
        gate_value = jax.nn.sigmoid(jnp.einsum('ijd,de->ije', gate_rows.astype(jnp.float32), gate_weight.astype(jnp.float32)))
        return (gate_value * update).astype(jnp.bfloat16)
    blocks_out = lax.map(row_block, jnp.arange(N_BLK, dtype=jnp.int32))
    return blocks_out.reshape(NRES, J, C)
```

```python
import functools

import jax
import jax.numpy as jnp
from jax import lax
from jax.experimental import pallas as pl
from jax.experimental.pallas import tpu as pltpu
from jax.sharding import PartitionSpec as P

JD = 13
PAD = 16
CHUNKS = 4
LAG = 2
EPS = 1e-05
F32 = jnp.float32
BF16 = jnp.bfloat16
NT = (((1,), (1,)), ((), ()))
TN = (((0,), (0,)), ((), ()))
NN = (((1,), (0,)), ((), ()))


def xor(a, b, n):
    total, bit = 0, 1
    while bit < n:
        total = total + bit * ((a // bit + b // bit) % 2)
        bit *= 2
    return total


def reverse_bits(t, n):
    total, bit = 0, 1
    while bit < n:
        total = total + (n // 2 // bit) * ((t // bit) % 2)
        bit *= 2
    return total


def sigmoid(x):
    return 0.5 * jnp.tanh(0.5 * x) + 0.5


def layer_norm(x, gain, bias):
    centre = jnp.mean(x, axis=-1, keepdims=True)
    centred = x - centre
    spread = jnp.mean(centred * centred, axis=-1, keepdims=True)
    return centred * lax.rsqrt(spread + EPS) * gain + bias


def gray(t, n):
    return xor(t, t // 2, n)


def groups():
    ends = [-(-JD * i // CHUNKS) for i in range(CHUNKS + 1)]
    return [(a, b - a) for a, b in zip(ends[:-1], ends[1:])]


def kernel(
    n_pos,
    slot_size,
    lens_hbm,
    pair_hbm,
    gain_hbm,
    bias_hbm,
    lgate_hbm,
    lvalue_hbm,
    rgate_hbm,
    rvalue_hbm,
    ogain_hbm,
    obias_hbm,
    oweight_hbm,
    gweight_hbm,
    out_hbm,
    lens,
    vectors,
    raw,
    pair,
    weights,
    right_all,
    left,
    r0,
    r1,
    work,
    send,
    own,
    recv,
    relay,
    gate_in,
    gate_val,
    out,
    load_sem,
    out_sem,
    rs_send,
    rs_recv,
    fw_send,
    fw_recv,
    ps_send,
    ps_recv,
    rl_send,
    rl_recv,
):
    rows, cols, ch = pair.shape
    hid = raw.shape[2]
    part = hid // CHUNKS
    pitch = 2 * rows + 8
    total = n_pos * CHUNKS
    last = n_pos - 1
    half = n_pos // 2
    blk = lax.axis_index("blk")
    z = lax.axis_index("chan")
    q = blk // 2
    h = blk % 2
    partner = 2 * q + 1 - h

    def load(n, src, dst):
        copy = pltpu.make_async_copy(src, dst, load_sem.at[n])
        copy.start()
        return copy

    first = [
        load(0, pair_hbm.at[pl.ds(0, JD)], pair.at[pl.ds(0, JD)]),
        load(1, rgate_hbm, raw.at[0]),
        load(2, rvalue_hbm, raw.at[1]),
        load(3, gain_hbm, vectors.at[pl.ds(0, 1)]),
        load(4, bias_hbm, vectors.at[pl.ds(8, 1)]),
        load(5, lens_hbm, lens),
    ]
    second = [
        load(6, pair_hbm.at[pl.ds(JD, rows - JD)], pair.at[pl.ds(JD, rows - JD)]),
        load(7, lgate_hbm, raw.at[2]),
        load(8, lvalue_hbm, raw.at[3]),
    ]
    third = [
        load(9, gweight_hbm, raw.at[4]),
        load(10, oweight_hbm, raw.at[5]),
        load(11, ogain_hbm, vectors.at[pl.ds(16, 1)]),
        load(12, obias_hbm, vectors.at[pl.ds(24, 1)]),
    ]

    barrier = pltpu.get_barrier_semaphore()
    for d in range(1, n_pos):
        pl.semaphore_signal(barrier, inc=1, device_id={"blk": 2 * xor(q, d, n_pos) + h})
        pl.semaphore_signal(barrier, inc=1, device_id={"chan": xor(z, d, n_pos)})
    pl.semaphore_signal(barrier, inc=1, device_id={"blk": partner})

    def turn(n):
        weights[n * hid : (n + 1) * hid, :] = raw[n].astype(F32).T.astype(BF16)

    for copy in first:
        copy.wait()
    turn(0)
    turn(1)

    col = z * cols + lax.broadcasted_iota(jnp.int32, (1, cols), 1)
    chain = col // slot_size
    chain_len = jnp.zeros_like(col)
    for s in range(lens.shape[0]):
        chain_len = jnp.where(chain == s, lens[s], chain_len)
    col_real = (col % slot_size < chain_len).astype(F32)

    def row_real(i):
        pos = blk * rows + i
        return jnp.where(pos % slot_size < lens[pos // slot_size], 1.0, 0.0).astype(F32)

    gain_v, bias_v = vectors[0:1, :], vectors[8:9, :]

    def norm_rows(i, count):
        x = pair[pl.ds(i, count)].astype(F32).reshape(count * cols, ch)
        return layer_norm(x, gain_v, bias_v).astype(BF16)

    for m in range(JD):
        normed = norm_rows(m, 1)
        mix = lax.dot_general(weights[: 2 * hid, :], normed, NT, preferred_element_type=F32)
        val = sigmoid(mix[:hid]) * mix[hid:] * (col_real * row_real(m))
        for k in range(CHUNKS):
            right_all[blk, k, m * part : (m + 1) * part, :] = val[
                k * part : (k + 1) * part
            ].astype(BF16)

    pl.semaphore_wait(barrier, 2 * (n_pos - 1) + 1)

    def right_copy(d, k):
        return pltpu.make_async_remote_copy(
            src_ref=right_all.at[blk, k],
            dst_ref=right_all.at[blk, k],
            send_sem=rs_send.at[d, k],
            recv_sem=rs_recv.at[d, k],
            device_id={"blk": 2 * xor(q, d, n_pos) + h},
        )

    def forward_copy(d, k):
        mine = 2 * xor(q, d, n_pos) + h
        return pltpu.make_async_remote_copy(
            src_ref=right_all.at[mine, k],
            dst_ref=right_all.at[mine, k],
            send_sem=fw_send.at[d, k],
            recv_sem=fw_recv.at[d, k],
            device_id={"blk": partner},
        )

    for hops in range(1, n_pos.bit_length()):
        for k in range(CHUNKS):
            for d in range(1, n_pos):
                if bin(d).count("1") == hops:
                    right_copy(d, k).start()
            if hops == 1:
                forward_copy(0, k).start()

    for copy in second:
        copy.wait()
    turn(2)
    turn(3)

    def left_rows(t, carry):
        i = 8 * t
        normed = norm_rows(i, 8)
        for u in range(8):
            for g in range(2):
                gate_in[pl.ds(g * rows + i + u, JD, stride=pitch), :] = normed[
                    u * cols + g * rows : u * cols + g * rows + JD
                ].astype(F32)
        mix = lax.dot_general(weights[2 * hid :, :], normed, NT, preferred_element_type=F32)
        val = sigmoid(mix[:hid]) * mix[hid:]
        for u in range(8):
            left[pl.ds(i + u, hid, stride=rows + 8), :] = val[:, u * cols : (u + 1) * cols] * (
                col_real * row_real(i + u)
            )
        return carry

    lax.fori_loop(0, rows // 8, left_rows, 0)

    def partial_copy(p, k):
        e = xor(z, p, n_pos)
        return pltpu.make_async_remote_copy(
            src_ref=send.at[p, k],
            dst_ref=recv.at[e, k],
            send_sem=ps_send.at[e, k],
            recv_sem=ps_recv.at[e, k],
            device_id={"chan": p},
        )

    def group_copy(p, n):
        start, count = groups()[n]
        here = pl.ds(start * part, count * part)
        return pltpu.make_async_remote_copy(
            src_ref=send.at[p, :, here],
            dst_ref=recv.at[1, :, here],
            send_sem=ps_send.at[1, n],
            recv_sem=ps_recv.at[1, n],
            device_id={"chan": p},
        )

    def relayed(source, p):
        return ((source == 0) & (p >= half)) | ((source == last) & (p < half))

    next_in = jnp.where(z == 0, 1, jnp.where(z == last, last - 1, -1))
    behind = jnp.where(z == 1, 0, jnp.where(z == last - 1, last, -1))

    def relay_copy(p, k):
        return pltpu.make_async_remote_copy(
            src_ref=send.at[p, k],
            dst_ref=relay.at[p, k],
            send_sem=rl_send.at[p, k],
            recv_sem=rl_recv.at[p, k],
            device_id={"chan": jnp.where(z < half, 1, last - 1)},
        )

    same_side = q // half == z // half

    def distance(t):
        d = gray(t, n_pos)
        return jnp.where(same_side, reverse_bits(d, n_pos), d)

    lag = jnp.where(same_side, LAG, CHUNKS + LAG)

    def pass_on(s, on):
        k = s % CHUNKS
        p = xor(q, distance(s // CHUNKS), n_pos)

        @pl.when(on & relayed(behind, p))
        def _():
            relay_copy(p, k).wait_recv()
            send[p, k] = (send[p, k].astype(F32) + relay[p, k].astype(F32)).astype(BF16)
            partial_copy(p, k).start()

    far = distance(last)

    def step(s, carry):
        t = s // CHUNKS
        k = s % CHUNKS
        d = distance(t)
        p = xor(q, d, n_pos)

        @pl.when((t > 0) & (t < last))
        def _():
            right_copy(d, k).wait_recv()
            forward_copy(d, k).start()

        forward_copy(d, k).wait_recv()
        for g, dst in enumerate((r0, r1)):
            for m in range(JD):
                dst[pl.ds(m, part, stride=PAD + 8), :] = right_all[
                    2 * p + g, k, m * part : (m + 1) * part, :
                ].astype(F32)

        base = pl.multiple_of(k * part * (rows + 8), 8)
        for c in range(part):
            rr = slice(c * (PAD + 8), c * (PAD + 8) + PAD)
            lhs = jnp.concatenate([r0[rr, :], r1[rr, :]], axis=0).astype(BF16)
            lc = left[pl.ds(base + c * (rows + 8), rows), :].astype(BF16)
            o = lax.dot_general(lhs, lc, NT, preferred_element_type=F32)
            work[pl.ds(c, PAD, stride=part + 8), :] = jnp.concatenate([o[:PAD], o[PAD:]], axis=1)

        @pl.when(p == z)
        def _():
            for m in range(JD):
                own[k, m * part : (m + 1) * part, :] = work[
                    m * (part + 8) : m * (part + 8) + part, :
                ]

        @pl.when(p != z)
        def _():
            for m in range(JD):
                send[p, k, m * part : (m + 1) * part, :] = work[
                    m * (part + 8) : m * (part + 8) + part, :
                ].astype(BF16)

            @pl.when(relayed(z, p))
            def _():
                relay_copy(p, k).start()

            later = (p == next_in) | relayed(behind, p)

            @pl.when(jnp.logical_not(relayed(z, p) | later))
            def _():
                partial_copy(p, k).start()

        @pl.when(t == 1)
        def _():
            right_copy(far, k).wait_recv()
            forward_copy(far, k).start()

        before = jnp.maximum(s - lag, 0)
        pass_on(before, s >= lag)
        return carry

    lax.fori_loop(0, total, step, 0)

    @pl.when(next_in >= 0)
    def _():
        for n in range(CHUNKS):
            group_copy(next_in, n).start()

    def rest(j, carry):
        pass_on(total - CHUNKS - LAG + j, CHUNKS + LAG - j <= lag)
        return carry

    lax.fori_loop(0, CHUNKS + LAG, rest, 0)

    for copy in third:
        copy.wait()

    def gates(m, carry):
        mix = lax.dot_general(
            gate_in[pl.ds(pl.multiple_of(m * pitch, 8), 2 * rows), :].astype(BF16),
            raw[4],
            NN,
            preferred_element_type=F32,
        )
        gate_val[m] = sigmoid(mix)
        return carry

    lax.fori_loop(0, JD, gates, 0)

    ogain_v = jnp.broadcast_to(vectors[16:17, :], (2 * rows, hid)).T
    obias_v = jnp.broadcast_to(vectors[24:25, :], (2 * rows, hid)).T
    for e in range(2, n_pos):
        source = xor(z, e, n_pos)

        @pl.when(jnp.logical_not(relayed(source, z)))
        def _():
            def gather(k, carry):
                partial_copy(source, k).wait_recv()
                own[k] = own[k] + recv[e, k].astype(F32)
                return carry

            lax.fori_loop(0, CHUNKS, gather, 0)

    inner = behind >= 0

    @pl.when(jnp.logical_not(inner))
    def _():
        for k in range(CHUNKS):
            partial_copy(xor(z, 1, n_pos), k).wait_recv()

    def finish(m):
        here = slice(m * part, (m + 1) * part)
        total = jnp.concatenate(
            [own[k, here, :] + recv[1, k, here, :].astype(F32) for k in range(CHUNKS)], axis=0
        )
        total = total.astype(BF16).astype(F32)
        centred = total - jnp.mean(total, axis=0, keepdims=True)
        spread = jnp.mean(centred * centred, axis=0, keepdims=True)
        normed = (centred * lax.rsqrt(spread + EPS) * ogain_v + obias_v).astype(BF16)
        val = lax.dot_general(normed, raw[5], TN, preferred_element_type=F32)
        val = (val * gate_val[m]).astype(BF16)
        for g in range(2):
            out[g * JD + m] = val[g * rows : (g + 1) * rows]

    def out_copy(n, g):
        start, count = groups()[n]
        here = pl.ds(g * JD + start, count)
        return pltpu.make_async_copy(out.at[here], out_hbm.at[here], out_sem.at[g, n])

    for n, (start, count) in enumerate(groups()):

        @pl.when(inner)
        def _():
            group_copy(behind, n).wait_recv()

        for m in range(start, start + count):
            finish(m)
        for g in range(2):
            out_copy(n, g).start()

    for n in range(CHUNKS):
        for g in range(2):
            out_copy(n, g).wait()

    def drain(s, carry):
        d = s // CHUNKS
        k = s % CHUNKS
        forward_copy(d, k).wait_send()

        @pl.when(d > 0)
        def _():
            target = xor(z, d, n_pos)
            right_copy(d, k).wait_send()

            @pl.when(relayed(z, target))
            def _():
                relay_copy(target, k).wait_send()

            @pl.when(jnp.logical_not(relayed(z, target) | (target == next_in)))
            def _():
                partial_copy(target, k).wait_send()

        return carry

    lax.fori_loop(0, total, drain, 0)

    @pl.when(next_in >= 0)
    def _():
        for n in range(CHUNKS):
            group_copy(next_in, n).wait_send()


def on_device(pair, lengths, gain, bias, lg, lv, rg, rv, ogain, obias, ow, gw):
    rows, cols, ch = pair.shape
    hid = lg.shape[1]
    n_blk = lax.axis_size("blk")
    n_pos = lax.axis_size("chan")
    assert n_blk == 2 * n_pos and cols == 2 * rows and n_pos >= 4 and n_pos & (n_pos - 1) == 0
    slot_size = rows * n_blk // lengths.shape[0]
    part = hid // CHUNKS
    sems = pltpu.SemaphoreType.DMA((n_pos, CHUNKS))
    block = (CHUNKS, JD * part, cols)
    result = pl.pallas_call(
        functools.partial(kernel, n_pos, slot_size),
        out_shape=jax.ShapeDtypeStruct((2 * JD, rows, ch), BF16),
        in_specs=[pl.BlockSpec(memory_space=pl.ANY)] * 12,
        out_specs=pl.BlockSpec(memory_space=pl.ANY),
        scratch_shapes=[
            pltpu.SMEM(lengths.shape, jnp.int32),
            pltpu.VMEM((32, ch), F32),
            pltpu.VMEM((6, ch, hid), BF16),
            pltpu.VMEM((rows, cols, ch), BF16),
            pltpu.VMEM((4 * hid, ch), BF16),
            pltpu.VMEM((n_blk,) + block, BF16),
            pltpu.VMEM((hid * (rows + 8), cols), F32),
            pltpu.VMEM((part * (PAD + 8), cols), F32),
            pltpu.VMEM((part * (PAD + 8), cols), F32),
            pltpu.VMEM((PAD * (part + 8), 2 * rows), F32),
            pltpu.VMEM((n_pos,) + block, BF16),
            pltpu.VMEM(block, F32),
            pltpu.VMEM((n_pos,) + block, BF16),
            pltpu.VMEM((n_pos,) + block, BF16),
            pltpu.VMEM((PAD * (2 * rows + 8), ch), F32),
            pltpu.VMEM((JD, 2 * rows, ch), F32),
            pltpu.VMEM((2 * JD, rows, ch), BF16),
            pltpu.SemaphoreType.DMA((13,)),
            pltpu.SemaphoreType.DMA((2, CHUNKS)),
        ]
        + [sems] * 8,
        compiler_params=pltpu.CompilerParams(
            collective_id=0, has_side_effects=True, vmem_limit_bytes=60 * 2**20
        ),
    )(
        lengths,
        pair,
        gain.reshape(1, ch),
        bias.reshape(1, ch),
        lg,
        lv,
        rg,
        rv,
        ogain.reshape(1, hid),
        obias.reshape(1, hid),
        ow,
        gw,
    )
    return jnp.transpose(result, (1, 0, 2))


def solution(mesh):
    in_specs = (P("blk", "chan", None),) + (P(),) * 11
    out_specs = P("blk", "chan", None)
    return jax.shard_map(
        on_device, mesh=mesh, in_specs=in_specs, out_specs=out_specs, check_vma=False
    )
```

```python
import functools

import jax
import jax.numpy as jnp
from jax import lax
from jax.experimental import pallas as pl
from jax.experimental.pallas import tpu as pltpu
from jax.sharding import PartitionSpec as P

JD = 13
PAD = 16
CHUNKS = 4
EPS = 1e-05
F32 = jnp.float32
BF16 = jnp.bfloat16
NT = (((1,), (1,)), ((), ()))
TN = (((0,), (0,)), ((), ()))
NN = (((1,), (0,)), ((), ()))


def xor(a, b, n):
    total, bit = 0, 1
    while bit < n:
        total = total + bit * ((a // bit + b // bit) % 2)
        bit *= 2
    return total


def reverse_bits(t, n):
    total, bit = 0, 1
    while bit < n:
        total = total + (n // 2 // bit) * ((t // bit) % 2)
        bit *= 2
    return total


def sigmoid(x):
    return 0.5 * jnp.tanh(0.5 * x) + 0.5


def layer_norm(x, gain, bias):
    centre = jnp.mean(x, axis=-1, keepdims=True)
    centred = x - centre
    spread = jnp.mean(centred * centred, axis=-1, keepdims=True)
    return centred * lax.rsqrt(spread + EPS) * gain + bias


def gray(t, n):
    return xor(t, t // 2, n)


def groups():
    ends = [-(-JD * i // CHUNKS) for i in range(CHUNKS + 1)]
    return [(a, b - a) for a, b in zip(ends[:-1], ends[1:])]


def kernel(
    n_pos,
    slot_size,
    lens_hbm,
    pair_hbm,
    gain_hbm,
    bias_hbm,
    lgate_hbm,
    lvalue_hbm,
    rgate_hbm,
    rvalue_hbm,
    ogain_hbm,
    obias_hbm,
    oweight_hbm,
    gweight_hbm,
    out_hbm,
    lens,
    vectors,
    raw,
    pair,
    weights,
    right_all,
    left,
    r0,
    r1,
    work,
    send,
    own,
    recv,
    relay,
    gate_in,
    gate_val,
    out,
    load_sem,
    out_sem,
    rs_send,
    rs_recv,
    fw_send,
    fw_recv,
    ps_send,
    ps_recv,
    rl_send,
    rl_recv,
):
    rows, cols, ch = pair.shape
    hid = raw.shape[2]
    part = hid // CHUNKS
    pitch = 2 * rows + 8
    total = n_pos * CHUNKS
    last = n_pos - 1
    half = n_pos // 2
    blk = lax.axis_index("blk")
    z = lax.axis_index("chan")
    q = blk // 2
    h = blk % 2
    partner = 2 * q + 1 - h

    def load(n, src, dst):
        copy = pltpu.make_async_copy(src, dst, load_sem.at[n])
        copy.start()
        return copy

    first = [
        load(0, pair_hbm.at[pl.ds(0, JD)], pair.at[pl.ds(0, JD)]),
        load(1, rgate_hbm, raw.at[0]),
        load(2, rvalue_hbm, raw.at[1]),
        load(3, gain_hbm, vectors.at[pl.ds(0, 1)]),
        load(4, bias_hbm, vectors.at[pl.ds(8, 1)]),
        load(5, lens_hbm, lens),
    ]
    second = [
        load(6, pair_hbm.at[pl.ds(JD, rows - JD)], pair.at[pl.ds(JD, rows - JD)]),
        load(7, lgate_hbm, raw.at[2]),
        load(8, lvalue_hbm, raw.at[3]),
    ]
    third = [
        load(9, gweight_hbm, raw.at[4]),
        load(10, oweight_hbm, raw.at[5]),
        load(11, ogain_hbm, vectors.at[pl.ds(16, 1)]),
        load(12, obias_hbm, vectors.at[pl.ds(24, 1)]),
    ]

    barrier = pltpu.get_barrier_semaphore()
    for d in range(1, n_pos):
        pl.semaphore_signal(barrier, inc=1, device_id={"blk": 2 * xor(q, d, n_pos) + h})
        pl.semaphore_signal(barrier, inc=1, device_id={"chan": xor(z, d, n_pos)})
    pl.semaphore_signal(barrier, inc=1, device_id={"blk": partner})

    def turn(n):
        weights[n * hid : (n + 1) * hid, :] = raw[n].astype(F32).T.astype(BF16)

    for copy in first:
        copy.wait()
    turn(0)
    turn(1)

    col = z * cols + lax.broadcasted_iota(jnp.int32, (1, cols), 1)
    chain = col // slot_size
    chain_len = jnp.zeros_like(col)
    for s in range(lens.shape[0]):
        chain_len = jnp.where(chain == s, lens[s], chain_len)
    col_real = (col % slot_size < chain_len).astype(F32)

    def row_real(i):
        pos = blk * rows + i
        return jnp.where(pos % slot_size < lens[pos // slot_size], 1.0, 0.0).astype(F32)

    gain_v, bias_v = vectors[0:1, :], vectors[8:9, :]

    def norm_rows(i, count):
        x = pair[pl.ds(i, count)].astype(F32).reshape(count * cols, ch)
        return layer_norm(x, gain_v, bias_v).astype(BF16)

    for m in range(JD):
        normed = norm_rows(m, 1)
        mix = lax.dot_general(weights[: 2 * hid, :], normed, NT, preferred_element_type=F32)
        val = sigmoid(mix[:hid]) * mix[hid:] * (col_real * row_real(m))
        for k in range(CHUNKS):
            right_all[blk, k, m * part : (m + 1) * part, :] = val[
                k * part : (k + 1) * part
            ].astype(BF16)

    pl.semaphore_wait(barrier, 2 * (n_pos - 1) + 1)

    def right_copy(d, k):
        return pltpu.make_async_remote_copy(
            src_ref=right_all.at[blk, k],
            dst_ref=right_all.at[blk, k],
            send_sem=rs_send.at[d, k],
            recv_sem=rs_recv.at[d, k],
            device_id={"blk": 2 * xor(q, d, n_pos) + h},
        )

    def forward_copy(d, k):
        mine = 2 * xor(q, d, n_pos) + h
        return pltpu.make_async_remote_copy(
            src_ref=right_all.at[mine, k],
            dst_ref=right_all.at[mine, k],
            send_sem=fw_send.at[d, k],
            recv_sem=fw_recv.at[d, k],
            device_id={"blk": partner},
        )

    for k in range(CHUNKS):
        for d in sorted(range(1, n_pos), key=int.bit_count):
            right_copy(d, k).start()
        forward_copy(0, k).start()

    for copy in second:
        copy.wait()
    turn(2)
    turn(3)

    def left_rows(t, carry):
        i = 8 * t
        normed = norm_rows(i, 8)
        for u in range(8):
            for g in range(2):
                gate_in[pl.ds(g * rows + i + u, JD, stride=pitch), :] = normed[
                    u * cols + g * rows : u * cols + g * rows + JD
                ].astype(F32)
        mix = lax.dot_general(weights[2 * hid :, :], normed, NT, preferred_element_type=F32)
        val = sigmoid(mix[:hid]) * mix[hid:]
        for u in range(8):
            left[pl.ds(i + u, hid, stride=rows + 8), :] = val[:, u * cols : (u + 1) * cols] * (
                col_real * row_real(i + u)
            )
        return carry

    lax.fori_loop(0, rows // 8, left_rows, 0)

    def partial_copy(p, k):
        e = xor(z, p, n_pos)
        return pltpu.make_async_remote_copy(
            src_ref=send.at[p, k],
            dst_ref=recv.at[e, k],
            send_sem=ps_send.at[e, k],
            recv_sem=ps_recv.at[e, k],
            device_id={"chan": p},
        )

    def group_copy(p, n):
        start, count = groups()[n]
        here = pl.ds(start * part, count * part)
        return pltpu.make_async_remote_copy(
            src_ref=send.at[p, :, here],
            dst_ref=recv.at[1, :, here],
            send_sem=ps_send.at[1, n],
            recv_sem=ps_recv.at[1, n],
            device_id={"chan": p},
        )

    def relayed(source, p):
        return ((source == 0) & (p >= half)) | ((source == last) & (p < half))

    next_in = jnp.where(z == 0, 1, jnp.where(z == last, last - 1, -1))
    behind = jnp.where(z == 1, 0, jnp.where(z == last - 1, last, -1))

    def relay_copy(p, k):
        return pltpu.make_async_remote_copy(
            src_ref=send.at[p, k],
            dst_ref=relay.at[p, k],
            send_sem=rl_send.at[p, k],
            recv_sem=rl_recv.at[p, k],
            device_id={"chan": jnp.where(z < half, 1, last - 1)},
        )

    same_side = q // half == z // half

    def side(d):
        return jnp.where(same_side, reverse_bits(d, n_pos), d)

    near, far = side(gray(1, n_pos)), side(gray(last, n_pos))

    def place(s):
        j = s % n_pos
        t = jnp.where(j < 2, j, jnp.where(j == 2, last, j - 1))
        return side(gray(t, n_pos)), s // n_pos

    def pass_on(s, on):
        d, k = place(s)
        p = xor(q, d, n_pos)

        @pl.when(on & relayed(behind, p))
        def _():
            relay_copy(p, k).wait_recv()
            send[p, k] = (send[p, k].astype(F32) + relay[p, k].astype(F32)).astype(BF16)
            partial_copy(p, k).start()

    def share(d, k):
        right_copy(d, k).wait_recv()
        forward_copy(d, k).start()

    def step(s, carry):
        d, k = place(s)
        p = xor(q, d, n_pos)
        opens = s % n_pos == 0

        @pl.when(opens & same_side)
        def _():
            share(near, k)
            share(far, k)

        @pl.when(s % n_pos > 2)
        def _():
            share(d, k)

        forward_copy(d, k).wait_recv()
        for g, dst in enumerate((r0, r1)):
            for m in range(JD):
                dst[pl.ds(m, part, stride=PAD + 8), :] = right_all[
                    2 * p + g, k, m * part : (m + 1) * part, :
                ].astype(F32)

        base = pl.multiple_of(k * part * (rows + 8), 8)
        for c in range(part):
            rr = slice(c * (PAD + 8), c * (PAD + 8) + PAD)
            lhs = jnp.concatenate([r0[rr, :], r1[rr, :]], axis=0).astype(BF16)
            lc = left[pl.ds(base + c * (rows + 8), rows), :].astype(BF16)
            o = lax.dot_general(lhs, lc, NT, preferred_element_type=F32)
            work[pl.ds(c, PAD, stride=part + 8), :] = jnp.concatenate([o[:PAD], o[PAD:]], axis=1)

        @pl.when(p == z)
        def _():
            for m in range(JD):
                own[k, m * part : (m + 1) * part, :] = work[
                    m * (part + 8) : m * (part + 8) + part, :
                ]

        @pl.when(p != z)
        def _():
            for m in range(JD):
                send[p, k, m * part : (m + 1) * part, :] = work[
                    m * (part + 8) : m * (part + 8) + part, :
                ].astype(BF16)

            @pl.when(relayed(z, p))
            def _():
                relay_copy(p, k).start()

            later = (p == next_in) | relayed(behind, p)

            @pl.when(jnp.logical_not(relayed(z, p) | later))
            def _():
                partial_copy(p, k).start()

        @pl.when(opens & jnp.logical_not(same_side))
        def _():
            share(near, k)
            share(far, k)

        pass_on(jnp.maximum(s - n_pos, 0), s >= n_pos)
        return carry

    lax.fori_loop(0, total, step, 0)

    @pl.when(next_in >= 0)
    def _():
        for n in range(CHUNKS):
            group_copy(next_in, n).start()

    def rest(j, carry):
        pass_on(total - n_pos + j, True)
        return carry

    lax.fori_loop(0, n_pos, rest, 0)

    for copy in third:
        copy.wait()

    def gates(m, carry):
        mix = lax.dot_general(
            gate_in[pl.ds(pl.multiple_of(m * pitch, 8), 2 * rows), :].astype(BF16),
            raw[4],
            NN,
            preferred_element_type=F32,
        )
        gate_val[m] = sigmoid(mix)
        return carry

    lax.fori_loop(0, JD, gates, 0)

    ogain_v = jnp.broadcast_to(vectors[16:17, :], (2 * rows, hid)).T
    obias_v = jnp.broadcast_to(vectors[24:25, :], (2 * rows, hid)).T
    for e in range(2, n_pos):
        source = xor(z, e, n_pos)

        @pl.when(jnp.logical_not(relayed(source, z)))
        def _():
            def gather(k, carry):
                partial_copy(source, k).wait_recv()
                own[k] = own[k] + recv[e, k].astype(F32)
                return carry

            lax.fori_loop(0, CHUNKS, gather, 0)

    fed = behind >= 0

    @pl.when(jnp.logical_not(fed))
    def _():
        for k in range(CHUNKS):
            partial_copy(xor(z, 1, n_pos), k).wait_recv()

    def finish(m):
        here = slice(m * part, (m + 1) * part)
        total = jnp.concatenate(
            [own[k, here, :] + recv[1, k, here, :].astype(F32) for k in range(CHUNKS)], axis=0
        )
        total = total.astype(BF16).astype(F32)
        centred = total - jnp.mean(total, axis=0, keepdims=True)
        spread = jnp.mean(centred * centred, axis=0, keepdims=True)
        normed = (centred * lax.rsqrt(spread + EPS) * ogain_v + obias_v).astype(BF16)
        val = lax.dot_general(normed, raw[5], TN, preferred_element_type=F32)
        val = (val * gate_val[m]).astype(BF16)
        for g in range(2):
            out[g * JD + m] = val[g * rows : (g + 1) * rows]

    def out_copy(n, g):
        start, count = groups()[n]
        here = pl.ds(g * JD + start, count)
        return pltpu.make_async_copy(out.at[here], out_hbm.at[here], out_sem.at[g, n])

    for n, (start, count) in enumerate(groups()):

        @pl.when(fed)
        def _():
            group_copy(behind, n).wait_recv()

        for m in range(start, start + count):
            finish(m)
        for g in range(2):
            out_copy(n, g).start()

    for n in range(CHUNKS):
        for g in range(2):
            out_copy(n, g).wait()

    def drain(s, carry):
        d = s // CHUNKS
        k = s % CHUNKS
        forward_copy(d, k).wait_send()

        @pl.when(d > 0)
        def _():
            target = xor(z, d, n_pos)
            right_copy(d, k).wait_send()

            @pl.when(relayed(z, target))
            def _():
                relay_copy(target, k).wait_send()

            @pl.when(jnp.logical_not(relayed(z, target) | (target == next_in)))
            def _():
                partial_copy(target, k).wait_send()

        return carry

    lax.fori_loop(0, total, drain, 0)

    @pl.when(next_in >= 0)
    def _():
        for n in range(CHUNKS):
            group_copy(next_in, n).wait_send()


def on_device(pair, lengths, gain, bias, lg, lv, rg, rv, ogain, obias, ow, gw):
    rows, cols, ch = pair.shape
    hid = lg.shape[1]
    n_blk = lax.axis_size("blk")
    n_pos = lax.axis_size("chan")
    assert n_blk == 2 * n_pos and cols == 2 * rows and n_pos >= 4 and n_pos & (n_pos - 1) == 0
    slot_size = rows * n_blk // lengths.shape[0]
    part = hid // CHUNKS
    sems = pltpu.SemaphoreType.DMA((n_pos, CHUNKS))
    block = (CHUNKS, JD * part, cols)
    result = pl.pallas_call(
        functools.partial(kernel, n_pos, slot_size),
        out_shape=jax.ShapeDtypeStruct((2 * JD, rows, ch), BF16),
        in_specs=[pl.BlockSpec(memory_space=pl.ANY)] * 12,
        out_specs=pl.BlockSpec(memory_space=pl.ANY),
        scratch_shapes=[
            pltpu.SMEM(lengths.shape, jnp.int32),
            pltpu.VMEM((32, ch), F32),
            pltpu.VMEM((6, ch, hid), BF16),
            pltpu.VMEM((rows, cols, ch), BF16),
            pltpu.VMEM((4 * hid, ch), BF16),
            pltpu.VMEM((n_blk,) + block, BF16),
            pltpu.VMEM((hid * (rows + 8), cols), F32),
            pltpu.VMEM((part * (PAD + 8), cols), F32),
            pltpu.VMEM((part * (PAD + 8), cols), F32),
            pltpu.VMEM((PAD * (part + 8), 2 * rows), F32),
            pltpu.VMEM((n_pos,) + block, BF16),
            pltpu.VMEM(block, F32),
            pltpu.VMEM((n_pos,) + block, BF16),
            pltpu.VMEM((n_pos,) + block, BF16),
            pltpu.VMEM((PAD * (2 * rows + 8), ch), F32),
            pltpu.VMEM((JD, 2 * rows, ch), F32),
            pltpu.VMEM((2 * JD, rows, ch), BF16),
            pltpu.SemaphoreType.DMA((13,)),
            pltpu.SemaphoreType.DMA((2, CHUNKS)),
        ]
        + [sems] * 8,
        compiler_params=pltpu.CompilerParams(
            collective_id=0, has_side_effects=True, vmem_limit_bytes=60 * 2**20
        ),
    )(
        lengths,
        pair,
        gain.reshape(1, ch),
        bias.reshape(1, ch),
        lg,
        lv,
        rg,
        rv,
        ogain.reshape(1, hid),
        obias.reshape(1, hid),
        ow,
        gw,
    )
    return jnp.transpose(result, (1, 0, 2))


def solution(mesh):
    in_specs = (P("blk", "chan", None),) + (P(),) * 11
    out_specs = P("blk", "chan", None)
    return jax.shard_map(
        on_device, mesh=mesh, in_specs=in_specs, out_specs=out_specs, check_vma=False
    )
```

```python
import functools

import jax
import jax.numpy as jnp
from jax import lax
from jax.experimental import pallas as pl
from jax.experimental.pallas import tpu as pltpu
from jax.sharding import PartitionSpec as P

JD = 13
PAD = 16
CHUNKS = 4
HOLD = 1
EPS = 1e-05
F32 = jnp.float32
BF16 = jnp.bfloat16
NT = (((1,), (1,)), ((), ()))
TN = (((0,), (0,)), ((), ()))
NN = (((1,), (0,)), ((), ()))


def xor(a, b, n):
    total, bit = 0, 1
    while bit < n:
        total = total + bit * ((a // bit + b // bit) % 2)
        bit *= 2
    return total


def reverse_bits(t, n):
    total, bit = 0, 1
    while bit < n:
        total = total + (n // 2 // bit) * ((t // bit) % 2)
        bit *= 2
    return total


def sigmoid(x):
    return 0.5 * jnp.tanh(0.5 * x) + 0.5


def layer_norm(x, gain, bias):
    centre = jnp.mean(x, axis=-1, keepdims=True)
    centred = x - centre
    spread = jnp.mean(centred * centred, axis=-1, keepdims=True)
    return centred * lax.rsqrt(spread + EPS) * gain + bias


def gray(t, n):
    return xor(t, t // 2, n)


def groups():
    ends = [-(-JD * i // CHUNKS) for i in range(CHUNKS + 1)]
    return [(a, b - a) for a, b in zip(ends[:-1], ends[1:])]


def kernel(
    n_pos,
    slot_size,
    lens_hbm,
    pair_hbm,
    gain_hbm,
    bias_hbm,
    lgate_hbm,
    lvalue_hbm,
    rgate_hbm,
    rvalue_hbm,
    ogain_hbm,
    obias_hbm,
    oweight_hbm,
    gweight_hbm,
    out,
    lens,
    vectors,
    raw,
    pair,
    weights,
    right_all,
    left,
    r0,
    r1,
    work,
    send,
    own,
    recv,
    relay,
    gate_in,
    gate_val,
    load_sem,
    sent,
    rs_recv,
    fw_recv,
    ps_recv,
    rl_recv,
):
    rows, cols, ch = pair.shape
    hid = raw.shape[2]
    part = hid // CHUNKS
    pitch = 2 * rows + 8
    total = n_pos * CHUNKS
    last = n_pos - 1
    half = n_pos // 2
    blk = lax.axis_index("blk")
    z = lax.axis_index("chan")
    q = blk // 2
    h = blk % 2
    partner = 2 * q + 1 - h

    def load(n, src, dst):
        copy = pltpu.make_async_copy(src, dst, load_sem.at[n])
        copy.start()
        return copy

    first = [
        load(0, pair_hbm.at[pl.ds(0, JD)], pair.at[pl.ds(0, JD)]),
        load(1, rgate_hbm, raw.at[0]),
        load(2, rvalue_hbm, raw.at[1]),
        load(3, gain_hbm, vectors.at[pl.ds(0, 1)]),
        load(4, bias_hbm, vectors.at[pl.ds(8, 1)]),
        load(5, lens_hbm, lens),
    ]
    second = [
        load(6, pair_hbm.at[pl.ds(JD, rows - JD)], pair.at[pl.ds(JD, rows - JD)]),
        load(7, lgate_hbm, raw.at[2]),
        load(8, lvalue_hbm, raw.at[3]),
    ]
    third = [
        load(9, gweight_hbm, raw.at[4]),
        load(10, oweight_hbm, raw.at[5]),
        load(11, ogain_hbm, vectors.at[pl.ds(16, 1)]),
        load(12, obias_hbm, vectors.at[pl.ds(24, 1)]),
    ]

    barrier = pltpu.get_barrier_semaphore()
    for d in range(1, n_pos):
        pl.semaphore_signal(barrier, inc=1, device_id={"blk": 2 * xor(q, d, n_pos) + h})
        pl.semaphore_signal(barrier, inc=1, device_id={"chan": xor(z, d, n_pos)})
    pl.semaphore_signal(barrier, inc=1, device_id={"blk": partner})

    def turn(n):
        weights[n * hid : (n + 1) * hid, :] = (0.5 * raw[n].astype(F32)).T.astype(BF16)

    for copy in first:
        copy.wait()
    turn(0)
    turn(1)

    col = z * cols + lax.broadcasted_iota(jnp.int32, (1, cols), 1)
    chain = col // slot_size
    chain_len = jnp.zeros_like(col)
    for s in range(lens.shape[0]):
        chain_len = jnp.where(chain == s, lens[s], chain_len)
    col_real = (col % slot_size < chain_len).astype(F32)

    def row_real(i):
        pos = blk * rows + i
        return jnp.where(pos % slot_size < lens[pos // slot_size], 1.0, 0.0).astype(F32)

    gain_v, bias_v = vectors[0:1, :] * ch**0.5, vectors[8:9, :]
    average = jnp.full((ch, ch), 1.0 / ch, BF16)

    def norm_rows(i, count, by_matmul):
        x = pair[pl.ds(i, count)].reshape(count * cols, ch)
        if by_matmul:
            centre = lax.dot_general(x, average, NN, preferred_element_type=F32)
        else:
            centre = jnp.mean(x.astype(F32), axis=-1, keepdims=True)
        centred = x.astype(F32) - centre
        spread = jnp.sum(centred * centred, axis=-1, keepdims=True)
        return (centred * lax.rsqrt(spread + ch * EPS) * gain_v + bias_v).astype(BF16)

    normed = norm_rows(0, JD, True)
    mix = lax.dot_general(weights[: 2 * hid, :], normed, NT, preferred_element_type=F32)
    val = (jnp.tanh(mix[:hid]) + 1.0) * mix[hid:]
    for m in range(JD):
        row = (val[:, m * cols : (m + 1) * cols] * (col_real * row_real(m))).astype(BF16)
        for k in range(CHUNKS):
            right_all[blk, k, m * part : (m + 1) * part, :] = row[k * part : (k + 1) * part]

    pl.semaphore_wait(barrier, 2 * (n_pos - 1) + 1)

    def right_copy(d, k):
        return pltpu.make_async_remote_copy(
            src_ref=right_all.at[blk, k],
            dst_ref=right_all.at[blk, k],
            send_sem=sent.at[0],
            recv_sem=rs_recv.at[d, k],
            device_id={"blk": 2 * xor(q, d, n_pos) + h},
        )

    def forward_copy(d, k):
        mine = 2 * xor(q, d, n_pos) + h
        return pltpu.make_async_remote_copy(
            src_ref=right_all.at[mine, k],
            dst_ref=right_all.at[mine, k],
            send_sem=sent.at[1],
            recv_sem=fw_recv.at[d, k],
            device_id={"blk": partner},
        )

    hops = sorted(range(1, n_pos), key=int.bit_count)
    close = n_pos.bit_length() - 1
    for d in hops[:close]:
        right_copy(d, 0).start()
    forward_copy(0, 0).start()

    def send_rest():
        for k in range(CHUNKS):
            for d in hops[close if k == 0 else 0 :]:
                right_copy(d, k).start()
            if k > 0:
                forward_copy(0, k).start()

    for copy in second:
        copy.wait()
    turn(2)
    turn(3)

    def left_rows(t, carry):
        i = 16 * t
        normed = norm_rows(i, 16, True)
        for u in range(16):
            for g in range(2):
                gate_in[pl.ds(g * rows + i + u, JD, stride=pitch), :] = normed[
                    u * cols + g * rows : u * cols + g * rows + JD
                ].astype(F32)
        mix = lax.dot_general(weights[2 * hid :, :], normed, NT, preferred_element_type=F32)
        val = (jnp.tanh(mix[:hid]) + 1.0) * mix[hid:]
        for u in range(16):
            left[pl.ds(i + u, hid, stride=rows + 8), :] = val[:, u * cols : (u + 1) * cols] * (
                col_real * row_real(i + u)
            )

        @pl.when(t == HOLD)
        def _():
            send_rest()

        return carry

    lax.fori_loop(0, rows // 16, left_rows, 0)

    def partial_copy(p, k):
        e = xor(z, p, n_pos)
        return pltpu.make_async_remote_copy(
            src_ref=send.at[p, k],
            dst_ref=recv.at[e, k],
            send_sem=sent.at[2],
            recv_sem=ps_recv.at[jnp.where(e == 1, n_pos + k, e)],
            device_id={"chan": p},
        )

    def group_copy(p, n):
        start, count = groups()[n]
        here = pl.ds(start * part, count * part)
        return pltpu.make_async_remote_copy(
            src_ref=send.at[p, :, here],
            dst_ref=recv.at[1, :, here],
            send_sem=sent.at[2],
            recv_sem=ps_recv.at[n_pos + n],
            device_id={"chan": p},
        )

    def relayed(source, p):
        return ((source == 0) & (p >= half)) | ((source == last) & (p < half))

    next_in = jnp.where(z == 0, 1, jnp.where(z == last, last - 1, -1))
    behind = jnp.where(z == 1, 0, jnp.where(z == last - 1, last, -1))

    def relay_copy(p, k):
        return pltpu.make_async_remote_copy(
            src_ref=send.at[p, k],
            dst_ref=relay.at[p, k],
            send_sem=sent.at[2],
            recv_sem=rl_recv.at[p % half, k],
            device_id={"chan": jnp.where(z < half, 1, last - 1)},
        )

    same_side = q // half == z // half

    def side(d):
        return jnp.where(same_side, reverse_bits(d, n_pos), d)

    near, far = side(gray(1, n_pos)), side(gray(last, n_pos))

    def place(s):
        j = s % n_pos
        t = jnp.where(j < 2, j, jnp.where(j == 2, last, j - 1))
        return side(gray(t, n_pos)), s // n_pos

    def pass_on(s, on):
        d, k = place(s)
        p = xor(q, d, n_pos)

        @pl.when(on & relayed(behind, p))
        def _():
            relay_copy(p, k).wait_recv()
            send[p, k] = (send[p, k].astype(F32) + relay[p, k].astype(F32)).astype(BF16)
            partial_copy(p, k).start()

    def share(d, k):
        right_copy(d, k).wait_recv()
        forward_copy(d, k).start()

    def step(s, carry):
        d, k = place(s)
        p = xor(q, d, n_pos)
        opens = s % n_pos == 0

        @pl.when(opens & same_side)
        def _():
            share(near, k)
            share(far, k)

        @pl.when(s % n_pos > 2)
        def _():
            share(d, k)

        forward_copy(d, k).wait_recv()
        for g, dst in enumerate((r0, r1)):
            for m in range(JD):
                dst[pl.ds(m, part, stride=PAD + 8), :] = right_all[
                    2 * p + g, k, m * part : (m + 1) * part, :
                ].astype(F32)

        base = pl.multiple_of(k * part * (rows + 8), 8)
        for c in range(part):
            rr = slice(c * (PAD + 8), c * (PAD + 8) + PAD)
            lhs = jnp.concatenate([r0[rr, :], r1[rr, :]], axis=0).astype(BF16)
            lc = left[pl.ds(base + c * (rows + 8), rows), :].astype(BF16)
            o = lax.dot_general(lhs, lc, NT, preferred_element_type=F32)
            work[pl.ds(c, PAD, stride=part + 8), :] = jnp.concatenate([o[:PAD], o[PAD:]], axis=1)

        @pl.when(p == z)
        def _():
            for m in range(JD):
                own[k, m * part : (m + 1) * part, :] = work[
                    m * (part + 8) : m * (part + 8) + part, :
                ]

        @pl.when(p != z)
        def _():
            for m in range(JD):
                send[p, k, m * part : (m + 1) * part, :] = work[
                    m * (part + 8) : m * (part + 8) + part, :
                ].astype(BF16)

            @pl.when(relayed(z, p))
            def _():
                relay_copy(p, k).start()

            later = (p == next_in) | relayed(behind, p)

            @pl.when(jnp.logical_not(relayed(z, p) | later))
            def _():
                partial_copy(p, k).start()

        @pl.when(opens & jnp.logical_not(same_side))
        def _():
            share(near, k)
            share(far, k)

        pass_on(jnp.maximum(s - n_pos, 0), s >= n_pos)
        return carry

    lax.fori_loop(0, total, step, 0)

    @pl.when(next_in >= 0)
    def _():
        for n in range(CHUNKS):
            group_copy(next_in, n).start()

    def rest(j, carry):
        pass_on(total - n_pos + j, True)
        return carry

    lax.fori_loop(0, n_pos, rest, 0)

    for copy in third:
        copy.wait()

    def gates(m, carry):
        mix = lax.dot_general(
            gate_in[pl.ds(pl.multiple_of(m * pitch, 8), 2 * rows), :].astype(BF16),
            raw[4],
            NN,
            preferred_element_type=F32,
        )
        gate_val[m] = sigmoid(mix)
        return carry

    lax.fori_loop(0, JD, gates, 0)

    ogain_v = jnp.broadcast_to(vectors[16:17, :], (2 * rows, hid)).T
    obias_v = jnp.broadcast_to(vectors[24:25, :], (2 * rows, hid)).T
    for e in range(2, n_pos):
        source = xor(z, e, n_pos)

        @pl.when(jnp.logical_not(relayed(source, z)))
        def _():
            pltpu.make_async_remote_copy(
                src_ref=send.at[source],
                dst_ref=recv.at[e],
                send_sem=sent.at[2],
                recv_sem=ps_recv.at[e],
                device_id={"chan": source},
            ).wait_recv()

            def gather(k, carry):
                own[k] = own[k] + recv[e, k].astype(F32)
                return carry

            lax.fori_loop(0, CHUNKS, gather, 0)

    fed = behind >= 0

    @pl.when(jnp.logical_not(fed))
    def _():
        for k in range(CHUNKS):
            partial_copy(xor(z, 1, n_pos), k).wait_recv()

    def finish(m):
        here = slice(m * part, (m + 1) * part)
        total = jnp.concatenate(
            [own[k, here, :] + recv[1, k, here, :].astype(F32) for k in range(CHUNKS)], axis=0
        )
        total = total.astype(BF16).astype(F32)
        centred = total - jnp.mean(total, axis=0, keepdims=True)
        spread = jnp.mean(centred * centred, axis=0, keepdims=True)
        normed = (centred * lax.rsqrt(spread + EPS) * ogain_v + obias_v).astype(BF16)
        val = lax.dot_general(normed, raw[5], TN, preferred_element_type=F32)
        val = (val * gate_val[m]).astype(BF16)
        for g in range(2):
            out[g * JD + m] = val[g * rows : (g + 1) * rows]

    for n, (start, count) in enumerate(groups()):

        @pl.when(fed)
        def _():
            group_copy(behind, n).wait_recv()

        for m in range(start, start + count):
            finish(m)
    def drain(n, blocks, buffer):
        here = buffer.at[pl.ds(0, blocks)]
        pltpu.make_async_remote_copy(
            src_ref=here,
            dst_ref=here,
            send_sem=sent.at[n],
            recv_sem=ps_recv.at[0],
            device_id={"blk": partner},
        ).wait_send()

    drain(0, n_pos - 1, right_all)
    drain(1, n_pos, right_all)
    drain(2, n_pos - 1, send)


def on_device(pair, lengths, gain, bias, lg, lv, rg, rv, ogain, obias, ow, gw):
    rows, cols, ch = pair.shape
    hid = lg.shape[1]
    n_blk = lax.axis_size("blk")
    n_pos = lax.axis_size("chan")
    assert n_blk == 2 * n_pos and cols == 2 * rows and n_pos >= 4 and n_pos & (n_pos - 1) == 0
    slot_size = rows * n_blk // lengths.shape[0]
    part = hid // CHUNKS
    block = (CHUNKS, JD * part, cols)
    operands = (
        lengths,
        pair,
        gain.reshape(1, ch),
        bias.reshape(1, ch),
        lg,
        lv,
        rg,
        rv,
        ogain.reshape(1, hid),
        obias.reshape(1, hid),
        ow,
        gw,
    )
    result = pl.pallas_call(
        functools.partial(kernel, n_pos, slot_size),
        out_shape=jax.ShapeDtypeStruct((2 * JD, rows, ch), BF16),
        in_specs=[pl.BlockSpec(memory_space=pl.ANY)] * 12,
        out_specs=pl.BlockSpec(memory_space=pltpu.VMEM),
        scratch_shapes=[
            pltpu.SMEM(lengths.shape, jnp.int32),
            pltpu.VMEM((32, ch), F32),
            pltpu.VMEM((6, ch, hid), BF16),
            pltpu.VMEM((rows, cols, ch), BF16),
            pltpu.VMEM((4 * hid, ch), BF16),
            pltpu.VMEM((n_blk,) + block, BF16),
            pltpu.VMEM((hid * (rows + 8), cols), F32),
            pltpu.VMEM((part * (PAD + 8), cols), F32),
            pltpu.VMEM((part * (PAD + 8), cols), F32),
            pltpu.VMEM((PAD * (part + 8), 2 * rows), F32),
            pltpu.VMEM((n_pos,) + block, BF16),
            pltpu.VMEM(block, F32),
            pltpu.VMEM((n_pos,) + block, BF16),
            pltpu.VMEM((n_pos,) + block, BF16),
            pltpu.VMEM((PAD * (2 * rows + 8), ch), F32),
            pltpu.VMEM((JD, 2 * rows, ch), F32),
            pltpu.SemaphoreType.DMA((13,)),
            pltpu.SemaphoreType.DMA((3,)),
            pltpu.SemaphoreType.DMA((n_pos, CHUNKS)),
            pltpu.SemaphoreType.DMA((n_pos, CHUNKS)),
            pltpu.SemaphoreType.DMA((n_pos + CHUNKS,)),
            pltpu.SemaphoreType.DMA((n_pos // 2, CHUNKS)),
        ],
        compiler_params=pltpu.CompilerParams(
            collective_id=0,
            has_side_effects=True,
            vmem_limit_bytes=(n_blk + 3 * n_pos) * 2 * JD * hid * cols + 16 * 2**20,
        ),
    )(*[pltpu.with_memory_space_constraint(x, pltpu.HBM) for x in operands])
    return jnp.transpose(result, (1, 0, 2))


def solution(mesh):
    in_specs = (P("blk", "chan", None),) + (P(),) * 11
    out_specs = P("blk", "chan", None)
    return jax.shard_map(
        on_device, mesh=mesh, in_specs=in_specs, out_specs=out_specs, check_vma=False
    )
```

```python
import functools

import jax
import jax.numpy as jnp
from jax import lax
from jax.experimental import pallas as pl
from jax.experimental.pallas import tpu as pltpu
from jax.sharding import PartitionSpec as P

JD = 13
PAD = 16
CHUNKS = 4
HOLD = 1
EPS = 1e-05
F32 = jnp.float32
BF16 = jnp.bfloat16
NT = (((1,), (1,)), ((), ()))
TN = (((0,), (0,)), ((), ()))
NN = (((1,), (0,)), ((), ()))


def xor(a, b, n):
    total, bit = 0, 1
    while bit < n:
        total = total + bit * ((a // bit + b // bit) % 2)
        bit *= 2
    return total


def reverse_bits(t, n):
    total, bit = 0, 1
    while bit < n:
        total = total + (n // 2 // bit) * ((t // bit) % 2)
        bit *= 2
    return total


def sigmoid(x):
    return 0.5 * jnp.tanh(0.5 * x) + 0.5


def layer_norm(x, gain, bias):
    centre = jnp.mean(x, axis=-1, keepdims=True)
    centred = x - centre
    spread = jnp.mean(centred * centred, axis=-1, keepdims=True)
    return centred * lax.rsqrt(spread + EPS) * gain + bias


def gray(t, n):
    return xor(t, t // 2, n)


GROUPS = ((0, 5), (5, 5), (10, 3))


def kernel(
    n_pos,
    slot_size,
    lens_hbm,
    pair_hbm,
    gain_hbm,
    bias_hbm,
    lgate_hbm,
    lvalue_hbm,
    rgate_hbm,
    rvalue_hbm,
    ogain_hbm,
    obias_hbm,
    oweight_hbm,
    gweight_hbm,
    out,
    lens,
    vectors,
    raw,
    pair,
    weights,
    right_all,
    left,
    r0,
    r1,
    work,
    send,
    own,
    recv,
    relay,
    gate_in,
    gate_val,
    load_sem,
    sent,
    rs_recv,
    fw_recv,
    ps_recv,
    rl_recv,
):
    rows, cols, ch = pair.shape
    hid = raw.shape[2]
    part = hid // CHUNKS
    pitch = 2 * rows + 8
    total = n_pos * CHUNKS
    last = n_pos - 1
    half = n_pos // 2
    blk = lax.axis_index("blk")
    z = lax.axis_index("chan")
    q = blk // 2
    h = blk % 2
    partner = 2 * q + 1 - h

    def load(n, src, dst):
        copy = pltpu.make_async_copy(src, dst, load_sem.at[n])
        copy.start()
        return copy

    first = [
        load(0, pair_hbm.at[pl.ds(0, JD)], pair.at[pl.ds(0, JD)]),
        load(1, rgate_hbm, raw.at[0]),
        load(2, rvalue_hbm, raw.at[1]),
        load(3, gain_hbm, vectors.at[pl.ds(0, 1)]),
        load(4, bias_hbm, vectors.at[pl.ds(8, 1)]),
        load(5, lens_hbm, lens),
    ]
    second = [
        load(6, pair_hbm.at[pl.ds(JD, rows - JD)], pair.at[pl.ds(JD, rows - JD)]),
        load(7, lgate_hbm, raw.at[2]),
        load(8, lvalue_hbm, raw.at[3]),
    ]
    third = [
        load(9, gweight_hbm, raw.at[4]),
        load(10, oweight_hbm, raw.at[5]),
        load(11, ogain_hbm, vectors.at[pl.ds(16, 1)]),
        load(12, obias_hbm, vectors.at[pl.ds(24, 1)]),
    ]

    barrier = pltpu.get_barrier_semaphore()
    for d in range(1, n_pos):
        pl.semaphore_signal(barrier, inc=1, device_id={"blk": 2 * xor(q, d, n_pos) + h})
        pl.semaphore_signal(barrier, inc=1, device_id={"chan": xor(z, d, n_pos)})
    pl.semaphore_signal(barrier, inc=1, device_id={"blk": partner})

    def turn(n):
        weights[n * hid : (n + 1) * hid, :] = (0.5 * raw[n].astype(F32)).T.astype(BF16)

    for copy in first:
        copy.wait()
    turn(0)
    turn(1)

    col = z * cols + lax.broadcasted_iota(jnp.int32, (1, cols), 1)
    chain = col // slot_size
    chain_len = jnp.zeros_like(col)
    for s in range(lens.shape[0]):
        chain_len = jnp.where(chain == s, lens[s], chain_len)
    col_real = (col % slot_size < chain_len).astype(F32)

    def row_real(i):
        pos = blk * rows + i
        return jnp.where(pos % slot_size < lens[pos // slot_size], 1.0, 0.0).astype(F32)

    gain_v, bias_v = vectors[0:1, :] * ch**0.5, vectors[8:9, :]
    average = jnp.full((ch, ch), 1.0 / ch, BF16)

    def norm_rows(i, count, by_matmul):
        x = pair[pl.ds(i, count)].reshape(count * cols, ch)
        if by_matmul:
            centre = lax.dot_general(x, average, NN, preferred_element_type=F32)
        else:
            centre = jnp.mean(x.astype(F32), axis=-1, keepdims=True)
        centred = x.astype(F32) - centre
        spread = jnp.sum(centred * centred, axis=-1, keepdims=True)
        return (centred * lax.rsqrt(spread + ch * EPS) * gain_v + bias_v).astype(BF16)

    normed = norm_rows(0, JD, True)
    mix = lax.dot_general(weights[: 2 * hid, :], normed, NT, preferred_element_type=F32)
    val = (jnp.tanh(mix[:hid]) + 1.0) * mix[hid:]
    for m in range(JD):
        row = (val[:, m * cols : (m + 1) * cols] * (col_real * row_real(m))).astype(BF16)
        for k in range(CHUNKS):
            right_all[blk, k, m * part : (m + 1) * part, :] = row[k * part : (k + 1) * part]

    pl.semaphore_wait(barrier, 2 * (n_pos - 1) + 1)

    def right_copy(d, k):
        return pltpu.make_async_remote_copy(
            src_ref=right_all.at[blk, k],
            dst_ref=right_all.at[blk, k],
            send_sem=sent.at[0],
            recv_sem=rs_recv.at[d, k],
            device_id={"blk": 2 * xor(q, d, n_pos) + h},
        )

    def forward_copy(d, k):
        mine = 2 * xor(q, d, n_pos) + h
        return pltpu.make_async_remote_copy(
            src_ref=right_all.at[mine, k],
            dst_ref=right_all.at[mine, k],
            send_sem=sent.at[1],
            recv_sem=fw_recv.at[d, k],
            device_id={"blk": partner},
        )

    hops = sorted(range(1, n_pos), key=int.bit_count)
    close = n_pos.bit_length() - 1
    for d in hops[:close]:
        right_copy(d, 0).start()
    forward_copy(0, 0).start()

    def send_rest():
        for k in range(CHUNKS):
            for d in hops[close if k == 0 else 0 :]:
                right_copy(d, k).start()
            if k > 0:
                forward_copy(0, k).start()

    for copy in second:
        copy.wait()
    turn(2)
    turn(3)

    def left_rows(t, carry):
        i = 16 * t
        normed = norm_rows(i, 16, True)
        for u in range(16):
            for g in range(2):
                gate_in[pl.ds(g * rows + i + u, JD, stride=pitch), :] = normed[
                    u * cols + g * rows : u * cols + g * rows + JD
                ].astype(F32)
        mix = lax.dot_general(weights[2 * hid :, :], normed, NT, preferred_element_type=F32)
        val = (jnp.tanh(mix[:hid]) + 1.0) * mix[hid:]
        for u in range(16):
            left[pl.ds(i + u, hid, stride=rows + 8), :] = val[:, u * cols : (u + 1) * cols] * (
                col_real * row_real(i + u)
            )

        @pl.when(t == HOLD)
        def _():
            send_rest()

        return carry

    lax.fori_loop(0, rows // 16, left_rows, 0)

    def partial_copy(p, k):
        e = xor(z, p, n_pos)
        return pltpu.make_async_remote_copy(
            src_ref=send.at[p, k],
            dst_ref=recv.at[e, k],
            send_sem=sent.at[2],
            recv_sem=ps_recv.at[jnp.where(e == 1, n_pos + k, e)],
            device_id={"chan": p},
        )

    def group_copy(p, n):
        start, count = GROUPS[n]
        here = pl.ds(start * part, count * part)
        return pltpu.make_async_remote_copy(
            src_ref=send.at[p, pl.ds(1, CHUNKS - 1), here],
            dst_ref=recv.at[1, pl.ds(1, CHUNKS - 1), here],
            send_sem=sent.at[2],
            recv_sem=ps_recv.at[n_pos + 1 + n],
            device_id={"chan": p},
        )

    def relayed(source, p):
        return ((source == 0) & (p >= half)) | ((source == last) & (p < half))

    next_in = jnp.where(z == 0, 1, jnp.where(z == last, last - 1, -1))
    behind = jnp.where(z == 1, 0, jnp.where(z == last - 1, last, -1))

    def relay_copy(p, k):
        return pltpu.make_async_remote_copy(
            src_ref=send.at[p, k],
            dst_ref=relay.at[p, k],
            send_sem=sent.at[2],
            recv_sem=rl_recv.at[p % half, k],
            device_id={"chan": jnp.where(z < half, 1, last - 1)},
        )

    same_side = q // half == z // half

    def side(d):
        return jnp.where(same_side, reverse_bits(d, n_pos), d)

    near, far = side(gray(1, n_pos)), side(gray(last, n_pos))

    def place(s):
        j = s % n_pos
        j = jnp.where((j < 3) & (q == z), (j + 1) % 3, j)
        t = jnp.where(j < 2, j, jnp.where(j == 2, last, j - 1))
        return side(gray(t, n_pos)), s // n_pos

    def pass_on(s, on):
        d, k = place(s)
        p = xor(q, d, n_pos)

        @pl.when(on & relayed(behind, p))
        def _():
            relay_copy(p, k).wait_recv()
            send[p, k] = (send[p, k].astype(F32) + relay[p, k].astype(F32)).astype(BF16)
            partial_copy(p, k).start()

    def share(d, k):
        right_copy(d, k).wait_recv()
        forward_copy(d, k).start()

    def step(s, carry):
        d, k = place(s)
        p = xor(q, d, n_pos)
        opens = s % n_pos == 0

        @pl.when(opens & (q == z))
        def _():
            share(near, k)
            share(far, k)

        @pl.when(s % n_pos > 2)
        def _():
            share(d, k)

        forward_copy(d, k).wait_recv()
        for g, dst in enumerate((r0, r1)):
            for m in range(JD):
                dst[pl.ds(m, part, stride=PAD + 8), :] = right_all[
                    2 * p + g, k, m * part : (m + 1) * part, :
                ].astype(F32)

        base = pl.multiple_of(k * part * (rows + 8), 8)
        for c in range(part):
            rr = slice(c * (PAD + 8), c * (PAD + 8) + PAD)
            lhs = jnp.concatenate([r0[rr, :], r1[rr, :]], axis=0).astype(BF16)
            lc = left[pl.ds(base + c * (rows + 8), rows), :].astype(BF16)
            o = lax.dot_general(lhs, lc, NT, preferred_element_type=F32)
            work[pl.ds(c, PAD, stride=part + 8), :] = jnp.concatenate([o[:PAD], o[PAD:]], axis=1)

        @pl.when(p == z)
        def _():
            for m in range(JD):
                own[k, m * part : (m + 1) * part, :] = work[
                    m * (part + 8) : m * (part + 8) + part, :
                ]

        @pl.when(p != z)
        def _():
            for m in range(JD):
                send[p, k, m * part : (m + 1) * part, :] = work[
                    m * (part + 8) : m * (part + 8) + part, :
                ].astype(BF16)

            @pl.when(relayed(z, p))
            def _():
                relay_copy(p, k).start()

            later = ((p == next_in) & (k > 0)) | relayed(behind, p)

            @pl.when(jnp.logical_not(relayed(z, p) | later))
            def _():
                partial_copy(p, k).start()

        @pl.when(opens & (q != z))
        def _():
            share(near, k)
            share(far, k)

        pass_on(jnp.maximum(s - n_pos, 0), s >= n_pos)
        return carry

    lax.fori_loop(0, total, step, 0)

    @pl.when(next_in >= 0)
    def _():
        for n in range(len(GROUPS)):
            group_copy(next_in, n).start()

    def rest(j, carry):
        pass_on(total - n_pos + j, True)
        return carry

    lax.fori_loop(0, n_pos, rest, 0)

    for copy in third:
        copy.wait()

    def gates(m, carry):
        mix = lax.dot_general(
            gate_in[pl.ds(pl.multiple_of(m * pitch, 8), 2 * rows), :].astype(BF16),
            raw[4],
            NN,
            preferred_element_type=F32,
        )
        gate_val[m] = sigmoid(mix)
        return carry

    lax.fori_loop(0, JD, gates, 0)

    ogain_v = jnp.broadcast_to(vectors[16:17, :], (2 * rows, hid)).T
    obias_v = jnp.broadcast_to(vectors[24:25, :], (2 * rows, hid)).T
    for e in range(2, n_pos):
        source = xor(z, e, n_pos)

        @pl.when(jnp.logical_not(relayed(source, z)))
        def _():
            pltpu.make_async_remote_copy(
                src_ref=send.at[source],
                dst_ref=recv.at[e],
                send_sem=sent.at[2],
                recv_sem=ps_recv.at[e],
                device_id={"chan": source},
            ).wait_recv()

            def gather(k, carry):
                own[k] = own[k] + recv[e, k].astype(F32)
                return carry

            lax.fori_loop(0, CHUNKS, gather, 0)

    fed = behind >= 0

    @pl.when(jnp.logical_not(fed))
    def _():
        for k in range(CHUNKS):
            partial_copy(xor(z, 1, n_pos), k).wait_recv()

    def finish(m):
        here = slice(m * part, (m + 1) * part)
        total = jnp.concatenate(
            [own[k, here, :] + recv[1, k, here, :].astype(F32) for k in range(CHUNKS)], axis=0
        )
        total = total.astype(BF16).astype(F32)
        centred = total - jnp.mean(total, axis=0, keepdims=True)
        spread = jnp.mean(centred * centred, axis=0, keepdims=True)
        normed = (centred * lax.rsqrt(spread + EPS) * ogain_v + obias_v).astype(BF16)
        val = lax.dot_general(normed, raw[5], TN, preferred_element_type=F32)
        val = (val * gate_val[m]).astype(BF16)
        for g in range(2):
            out[g * JD + m] = val[g * rows : (g + 1) * rows]

    @pl.when(fed)
    def _():
        partial_copy(behind, 0).wait_recv()

    for n, (start, count) in enumerate(GROUPS):

        @pl.when(fed)
        def _():
            group_copy(behind, n).wait_recv()

        for m in range(start, start + count):
            finish(m)
    def drain(n, blocks, buffer):
        here = buffer.at[pl.ds(0, blocks)]
        pltpu.make_async_remote_copy(
            src_ref=here,
            dst_ref=here,
            send_sem=sent.at[n],
            recv_sem=ps_recv.at[0],
            device_id={"blk": partner},
        ).wait_send()

    drain(0, n_pos - 1, right_all)
    drain(1, n_pos, right_all)
    drain(2, n_pos - 1, send)


def on_device(pair, lengths, gain, bias, lg, lv, rg, rv, ogain, obias, ow, gw):
    rows, cols, ch = pair.shape
    hid = lg.shape[1]
    n_blk = lax.axis_size("blk")
    n_pos = lax.axis_size("chan")
    assert n_blk == 2 * n_pos and cols == 2 * rows and n_pos >= 4 and n_pos & (n_pos - 1) == 0
    slot_size = rows * n_blk // lengths.shape[0]
    part = hid // CHUNKS
    block = (CHUNKS, JD * part, cols)
    operands = (
        lengths,
        pair,
        gain.reshape(1, ch),
        bias.reshape(1, ch),
        lg,
        lv,
        rg,
        rv,
        ogain.reshape(1, hid),
        obias.reshape(1, hid),
        ow,
        gw,
    )
    result = pl.pallas_call(
        functools.partial(kernel, n_pos, slot_size),
        out_shape=jax.ShapeDtypeStruct((2 * JD, rows, ch), BF16),
        in_specs=[pl.BlockSpec(memory_space=pl.ANY)] * 12,
        out_specs=pl.BlockSpec(memory_space=pltpu.VMEM),
        scratch_shapes=[
            pltpu.SMEM(lengths.shape, jnp.int32),
            pltpu.VMEM((32, ch), F32),
            pltpu.VMEM((6, ch, hid), BF16),
            pltpu.VMEM((rows, cols, ch), BF16),
            pltpu.VMEM((4 * hid, ch), BF16),
            pltpu.VMEM((n_blk,) + block, BF16),
            pltpu.VMEM((hid * (rows + 8), cols), F32),
            pltpu.VMEM((part * (PAD + 8), cols), F32),
            pltpu.VMEM((part * (PAD + 8), cols), F32),
            pltpu.VMEM((PAD * (part + 8), 2 * rows), F32),
            pltpu.VMEM((n_pos,) + block, BF16),
            pltpu.VMEM(block, F32),
            pltpu.VMEM((n_pos,) + block, BF16),
            pltpu.VMEM((n_pos,) + block, BF16),
            pltpu.VMEM((PAD * (2 * rows + 8), ch), F32),
            pltpu.VMEM((JD, 2 * rows, ch), F32),
            pltpu.SemaphoreType.DMA((13,)),
            pltpu.SemaphoreType.DMA((3,)),
            pltpu.SemaphoreType.DMA((n_pos, CHUNKS)),
            pltpu.SemaphoreType.DMA((n_pos, CHUNKS)),
            pltpu.SemaphoreType.DMA((n_pos + CHUNKS,)),
            pltpu.SemaphoreType.DMA((n_pos // 2, CHUNKS)),
        ],
        compiler_params=pltpu.CompilerParams(
            collective_id=0,
            has_side_effects=True,
            vmem_limit_bytes=(n_blk + 3 * n_pos) * 2 * JD * hid * cols + 16 * 2**20,
        ),
    )(*[pltpu.with_memory_space_constraint(x, pltpu.HBM) for x in operands])
    return jnp.transpose(result, (1, 0, 2))


def solution(mesh):
    in_specs = (P("blk", "chan", None),) + (P(),) * 11
    out_specs = P("blk", "chan", None)
    return jax.shard_map(
        on_device, mesh=mesh, in_specs=in_specs, out_specs=out_specs, check_vma=False
    )
```

```python
import functools

import jax
import jax.numpy as jnp
from jax import lax
from jax.experimental import pallas as pl
from jax.experimental.pallas import tpu as pltpu
from jax.sharding import PartitionSpec as P

JD = 13
PAD = 16
CHUNKS = 4
HOLD = 1
EPS = 1e-05
F32 = jnp.float32
BF16 = jnp.bfloat16
NT = (((1,), (1,)), ((), ()))
TN = (((0,), (0,)), ((), ()))
NN = (((1,), (0,)), ((), ()))


def xor(a, b, n):
    total, bit = 0, 1
    while bit < n:
        total = total + bit * ((a // bit + b // bit) % 2)
        bit *= 2
    return total


def reverse_bits(t, n):
    total, bit = 0, 1
    while bit < n:
        total = total + (n // 2 // bit) * ((t // bit) % 2)
        bit *= 2
    return total


def sigmoid(x):
    return 0.5 * jnp.tanh(0.5 * x) + 0.5


def layer_norm(x, gain, bias):
    centre = jnp.mean(x, axis=-1, keepdims=True)
    centred = x - centre
    spread = jnp.mean(centred * centred, axis=-1, keepdims=True)
    return centred * lax.rsqrt(spread + EPS) * gain + bias


def gray(t, n):
    return xor(t, t // 2, n)


GROUPS = ((0, 5), (5, 5), (10, 3))


def kernel(
    n_pos,
    slot_size,
    lens_hbm,
    pair_hbm,
    gain_hbm,
    bias_hbm,
    lgate_hbm,
    lvalue_hbm,
    rgate_hbm,
    rvalue_hbm,
    ogain_hbm,
    obias_hbm,
    oweight_hbm,
    gweight_hbm,
    out,
    lens,
    vectors,
    raw,
    pair,
    weights,
    right_all,
    left,
    r0,
    r1,
    work,
    send,
    own,
    recv,
    relay,
    gate_in,
    gate_val,
    load_sem,
    sent,
    rs_recv,
    fw_recv,
    ps_recv,
    rl_recv,
    ready,
):
    rows, cols, ch = pair.shape
    hid = raw.shape[2]
    part = hid // CHUNKS
    pitch = 2 * rows + 8
    total = n_pos * CHUNKS
    last = n_pos - 1
    half = n_pos // 2
    blk = lax.axis_index("blk")
    z = lax.axis_index("chan")
    q = blk // 2
    h = blk % 2
    partner = 2 * q + 1 - h

    def load(n, src, dst):
        copy = pltpu.make_async_copy(src, dst, load_sem.at[n])
        copy.start()
        return copy

    first = [
        load(0, pair_hbm.at[pl.ds(0, JD)], pair.at[pl.ds(0, JD)]),
        load(1, rgate_hbm, raw.at[0]),
        load(2, rvalue_hbm, raw.at[1]),
        load(3, gain_hbm, vectors.at[pl.ds(0, 1)]),
        load(4, bias_hbm, vectors.at[pl.ds(8, 1)]),
        load(5, lens_hbm, lens),
    ]
    second = [
        load(6, pair_hbm.at[pl.ds(JD, rows - JD)], pair.at[pl.ds(JD, rows - JD)]),
        load(7, lgate_hbm, raw.at[2]),
        load(8, lvalue_hbm, raw.at[3]),
    ]
    third = [
        load(9, gweight_hbm, raw.at[4]),
        load(10, oweight_hbm, raw.at[5]),
        load(11, ogain_hbm, vectors.at[pl.ds(16, 1)]),
        load(12, obias_hbm, vectors.at[pl.ds(24, 1)]),
    ]

    def relayed(source, p):
        return ((source == 0) & (p >= half)) | ((source == last) & (p < half))

    def across(source, p):
        return ((source == 1) & (p == last)) | ((source == last - 1) & (p == 0))

    next_in = jnp.where(z == 0, 1, jnp.where(z == last, last - 1, -1))
    behind = jnp.where(z == 1, 0, jnp.where(z == last - 1, last, -1))

    fed = behind >= 0
    barrier = pltpu.get_barrier_semaphore()
    for d in range(1, n_pos):
        pl.semaphore_signal(barrier, inc=1, device_id={"blk": 2 * xor(q, d, n_pos) + h})
        source = xor(z, d, n_pos)

        @pl.when(jnp.logical_not(relayed(source, z) | across(source, z)))
        def _():
            pl.semaphore_signal(barrier, inc=1, device_id={"chan": source})

    pl.semaphore_signal(barrier, inc=1, device_id={"blk": partner})

    def turn(n):
        weights[n * hid : (n + 1) * hid, :] = (0.5 * raw[n].astype(F32)).T.astype(BF16)

    for copy in first:
        copy.wait()
    turn(0)
    turn(1)

    col = z * cols + lax.broadcasted_iota(jnp.int32, (1, cols), 1)
    chain = col // slot_size
    chain_len = jnp.zeros_like(col)
    for s in range(lens.shape[0]):
        chain_len = jnp.where(chain == s, lens[s], chain_len)
    col_real = (col % slot_size < chain_len).astype(F32)

    def row_real(i):
        pos = blk * rows + i
        return jnp.where(pos % slot_size < lens[pos // slot_size], 1.0, 0.0).astype(F32)

    gain_v, bias_v = vectors[0:1, :] * ch**0.5, vectors[8:9, :]
    average = jnp.full((ch, ch), 1.0 / ch, BF16)

    def norm_rows(i, count, by_matmul):
        x = pair[pl.ds(i, count)].reshape(count * cols, ch)
        if by_matmul:
            centre = lax.dot_general(x, average, NN, preferred_element_type=F32)
        else:
            centre = jnp.mean(x.astype(F32), axis=-1, keepdims=True)
        centred = x.astype(F32) - centre
        spread = jnp.sum(centred * centred, axis=-1, keepdims=True)
        return (centred * lax.rsqrt(spread + ch * EPS) * gain_v + bias_v).astype(BF16)

    normed = norm_rows(0, JD, True)
    mix = lax.dot_general(weights[: 2 * hid, :], normed, NT, preferred_element_type=F32)
    val = (jnp.tanh(mix[:hid]) + 1.0) * mix[hid:]
    for m in range(JD):
        row = (val[:, m * cols : (m + 1) * cols] * (col_real * row_real(m))).astype(BF16)
        for k in range(CHUNKS):
            right_all[blk, k, m * part : (m + 1) * part, :] = row[k * part : (k + 1) * part]

    direct = jnp.where(next_in >= 0, half - 1, jnp.where(fed, last - 1, last))
    pl.semaphore_wait(barrier, direct + n_pos)

    @pl.when(fed)
    def _():
        pl.semaphore_signal(ready, inc=1, device_id={"chan": last - z})


    def right_copy(d, k):
        return pltpu.make_async_remote_copy(
            src_ref=right_all.at[blk, k],
            dst_ref=right_all.at[blk, k],
            send_sem=sent.at[0],
            recv_sem=rs_recv.at[d, k],
            device_id={"blk": 2 * xor(q, d, n_pos) + h},
        )

    def forward_copy(d, k):
        mine = 2 * xor(q, d, n_pos) + h
        return pltpu.make_async_remote_copy(
            src_ref=right_all.at[mine, k],
            dst_ref=right_all.at[mine, k],
            send_sem=sent.at[1],
            recv_sem=fw_recv.at[d, k],
            device_id={"blk": partner},
        )

    hops = sorted(range(1, n_pos), key=int.bit_count)
    close = n_pos.bit_length() - 1
    for d in hops[:close]:
        right_copy(d, 0).start()
    forward_copy(0, 0).start()

    def send_rest():
        for k in range(CHUNKS):
            for d in hops[close if k == 0 else 0 :]:
                right_copy(d, k).start()
            if k > 0:
                forward_copy(0, k).start()

    for copy in second:
        copy.wait()
    turn(2)
    turn(3)

    def left_rows(t, carry):
        i = 16 * t
        normed = norm_rows(i, 16, True)
        for u in range(16):
            for g in range(2):
                gate_in[pl.ds(g * rows + i + u, JD, stride=pitch), :] = normed[
                    u * cols + g * rows : u * cols + g * rows + JD
                ].astype(F32)
        mix = lax.dot_general(weights[2 * hid :, :], normed, NT, preferred_element_type=F32)
        val = (jnp.tanh(mix[:hid]) + 1.0) * mix[hid:]
        for u in range(16):
            left[pl.ds(i + u, hid, stride=rows + 8), :] = val[:, u * cols : (u + 1) * cols] * (
                col_real * row_real(i + u)
            )

        @pl.when(t == HOLD)
        def _():
            send_rest()

        return carry

    lax.fori_loop(0, rows // 16, left_rows, 0)

    @pl.when(fed)
    def _():
        pl.semaphore_wait(ready, 1)

    def partial_copy(p, k):
        e = xor(z, p, n_pos)
        return pltpu.make_async_remote_copy(
            src_ref=send.at[p, k],
            dst_ref=recv.at[e, k],
            send_sem=sent.at[2],
            recv_sem=ps_recv.at[jnp.where(e == 1, n_pos + k, e)],
            device_id={"chan": p},
        )

    def group_copy(p, n):
        start, count = GROUPS[n]
        here = pl.ds(start * part, count * part)
        return pltpu.make_async_remote_copy(
            src_ref=send.at[p, pl.ds(1, CHUNKS - 1), here],
            dst_ref=recv.at[1, pl.ds(1, CHUNKS - 1), here],
            send_sem=sent.at[2],
            recv_sem=ps_recv.at[n_pos + 1 + n],
            device_id={"chan": p},
        )

    def relay_copy(p, k):
        return pltpu.make_async_remote_copy(
            src_ref=send.at[p, k],
            dst_ref=relay.at[p, k],
            send_sem=sent.at[2],
            recv_sem=rl_recv.at[p % half, k],
            device_id={"chan": jnp.where(z < half, 1, last - 1)},
        )

    same_side = q // half == z // half

    def side(d):
        return jnp.where(same_side, reverse_bits(d, n_pos), d)

    near, far = side(gray(1, n_pos)), side(gray(last, n_pos))

    def place(s):
        j = s % n_pos
        j = jnp.where((j < 3) & (q == z), (j + 1) % 3, j)
        t = jnp.where(j < 2, j, jnp.where(j == 2, last, j - 1))
        return side(gray(t, n_pos)), s // n_pos

    def pass_on(s, on):
        d, k = place(s)
        p = xor(q, d, n_pos)

        @pl.when(on & relayed(behind, p))
        def _():
            relay_copy(p, k).wait_recv()
            send[p, k] = (send[p, k].astype(F32) + relay[p, k].astype(F32)).astype(BF16)
            partial_copy(p, k).start()

    def share(d, k):
        right_copy(d, k).wait_recv()
        forward_copy(d, k).start()

    def step(s, carry):
        d, k = place(s)
        p = xor(q, d, n_pos)
        opens = s % n_pos == 0

        @pl.when(opens & (q == z))
        def _():
            share(near, k)
            share(far, k)

        @pl.when(s % n_pos > 2)
        def _():
            share(d, k)

        forward_copy(d, k).wait_recv()
        for g, dst in enumerate((r0, r1)):
            for m in range(JD):
                dst[pl.ds(m, part, stride=PAD + 8), :] = right_all[
                    2 * p + g, k, m * part : (m + 1) * part, :
                ].astype(F32)

        base = pl.multiple_of(k * part * (rows + 8), 8)
        for c in range(part):
            rr = slice(c * (PAD + 8), c * (PAD + 8) + PAD)
            lhs = jnp.concatenate([r0[rr, :], r1[rr, :]], axis=0).astype(BF16)
            lc = left[pl.ds(base + c * (rows + 8), rows), :].astype(BF16)
            o = lax.dot_general(lhs, lc, NT, preferred_element_type=F32)
            work[pl.ds(c, PAD, stride=part + 8), :] = jnp.concatenate([o[:PAD], o[PAD:]], axis=1)

        @pl.when(p == z)
        def _():
            for m in range(JD):
                own[k, m * part : (m + 1) * part, :] = work[
                    m * (part + 8) : m * (part + 8) + part, :
                ]

        @pl.when(p != z)
        def _():
            for m in range(JD):
                send[p, k, m * part : (m + 1) * part, :] = work[
                    m * (part + 8) : m * (part + 8) + part, :
                ].astype(BF16)

            @pl.when(relayed(z, p))
            def _():
                relay_copy(p, k).start()

            later = ((p == next_in) & ((k > 0) | jnp.logical_not(same_side))) | relayed(behind, p)

            @pl.when(jnp.logical_not(relayed(z, p) | later))
            def _():
                partial_copy(p, k).start()

        @pl.when(opens & (q != z))
        def _():
            share(near, k)

            @pl.when(k > 0)
            def _():
                share(far, k)

        @pl.when((s == 1) & (q != z))
        def _():
            share(far, 0)

        pass_on(jnp.maximum(s - n_pos, 0), s >= n_pos)
        return carry

    lax.fori_loop(0, total, step, 0)

    @pl.when((next_in >= 0) & jnp.logical_not(same_side))
    def _():
        partial_copy(next_in, 0).start()

    @pl.when(next_in >= 0)
    def _():
        for n in range(len(GROUPS)):
            group_copy(next_in, n).start()

    def rest(j, carry):
        pass_on(total - n_pos + j, True)
        return carry

    lax.fori_loop(0, n_pos, rest, 0)

    for copy in third:
        copy.wait()

    def gates(m, carry):
        mix = lax.dot_general(
            gate_in[pl.ds(pl.multiple_of(m * pitch, 8), 2 * rows), :].astype(BF16),
            raw[4],
            NN,
            preferred_element_type=F32,
        )
        gate_val[m] = sigmoid(mix)
        return carry

    lax.fori_loop(0, JD, gates, 0)

    ogain_v = jnp.broadcast_to(vectors[16:17, :], (2 * rows, hid)).T
    obias_v = jnp.broadcast_to(vectors[24:25, :], (2 * rows, hid)).T
    for e in range(2, n_pos):
        source = xor(z, e, n_pos)

        @pl.when(jnp.logical_not(relayed(source, z)))
        def _():
            pltpu.make_async_remote_copy(
                src_ref=send.at[source],
                dst_ref=recv.at[e],
                send_sem=sent.at[2],
                recv_sem=ps_recv.at[e],
                device_id={"chan": source},
            ).wait_recv()

            def gather(k, carry):
                own[k] = own[k] + recv[e, k].astype(F32)
                return carry

            lax.fori_loop(0, CHUNKS, gather, 0)

    @pl.when(jnp.logical_not(fed))
    def _():
        for k in range(CHUNKS):
            partial_copy(xor(z, 1, n_pos), k).wait_recv()

    def finish(m):
        here = slice(m * part, (m + 1) * part)
        total = jnp.concatenate(
            [own[k, here, :] + recv[1, k, here, :].astype(F32) for k in range(CHUNKS)], axis=0
        )
        total = total.astype(BF16).astype(F32)
        centred = total - jnp.mean(total, axis=0, keepdims=True)
        spread = jnp.mean(centred * centred, axis=0, keepdims=True)
        normed = (centred * lax.rsqrt(spread + EPS) * ogain_v + obias_v).astype(BF16)
        val = lax.dot_general(normed, raw[5], TN, preferred_element_type=F32)
        val = (val * gate_val[m]).astype(BF16)
        for g in range(2):
            out[g * JD + m] = val[g * rows : (g + 1) * rows]

    @pl.when(fed)
    def _():
        partial_copy(behind, 0).wait_recv()

    for n, (start, count) in enumerate(GROUPS):

        @pl.when(fed)
        def _():
            group_copy(behind, n).wait_recv()

        for m in range(start, start + count):
            finish(m)
    def drain(n, blocks, buffer):
        here = buffer.at[pl.ds(0, blocks)]
        pltpu.make_async_remote_copy(
            src_ref=here,
            dst_ref=here,
            send_sem=sent.at[n],
            recv_sem=ps_recv.at[0],
            device_id={"blk": partner},
        ).wait_send()

    drain(0, n_pos - 1, right_all)
    drain(1, n_pos, right_all)
    drain(2, n_pos - 1, send)


def on_device(pair, lengths, gain, bias, lg, lv, rg, rv, ogain, obias, ow, gw):
    rows, cols, ch = pair.shape
    hid = lg.shape[1]
    n_blk = lax.axis_size("blk")
    n_pos = lax.axis_size("chan")
    assert n_blk == 2 * n_pos and cols == 2 * rows and n_pos >= 4 and n_pos & (n_pos - 1) == 0
    slot_size = rows * n_blk // lengths.shape[0]
    part = hid // CHUNKS
    block = (CHUNKS, JD * part, cols)
    operands = (
        lengths,
        pair,
        gain.reshape(1, ch),
        bias.reshape(1, ch),
        lg,
        lv,
        rg,
        rv,
        ogain.reshape(1, hid),
        obias.reshape(1, hid),
        ow,
        gw,
    )
    result = pl.pallas_call(
        functools.partial(kernel, n_pos, slot_size),
        out_shape=jax.ShapeDtypeStruct((2 * JD, rows, ch), BF16),
        in_specs=[pl.BlockSpec(memory_space=pl.ANY)] * 12,
        out_specs=pl.BlockSpec(memory_space=pltpu.VMEM),
        scratch_shapes=[
            pltpu.SMEM(lengths.shape, jnp.int32),
            pltpu.VMEM((32, ch), F32),
            pltpu.VMEM((6, ch, hid), BF16),
            pltpu.VMEM((rows, cols, ch), BF16),
            pltpu.VMEM((4 * hid, ch), BF16),
            pltpu.VMEM((n_blk,) + block, BF16),
            pltpu.VMEM((hid * (rows + 8), cols), F32),
            pltpu.VMEM((part * (PAD + 8), cols), F32),
            pltpu.VMEM((part * (PAD + 8), cols), F32),
            pltpu.VMEM((PAD * (part + 8), 2 * rows), F32),
            pltpu.VMEM((n_pos,) + block, BF16),
            pltpu.VMEM(block, F32),
            pltpu.VMEM((n_pos,) + block, BF16),
            pltpu.VMEM((n_pos,) + block, BF16),
            pltpu.VMEM((PAD * (2 * rows + 8), ch), F32),
            pltpu.VMEM((JD, 2 * rows, ch), F32),
            pltpu.SemaphoreType.DMA((13,)),
            pltpu.SemaphoreType.DMA((3,)),
            pltpu.SemaphoreType.DMA((n_pos, CHUNKS)),
            pltpu.SemaphoreType.DMA((n_pos, CHUNKS)),
            pltpu.SemaphoreType.DMA((n_pos + CHUNKS,)),
            pltpu.SemaphoreType.DMA((n_pos // 2, CHUNKS)),
            pltpu.SemaphoreType.REGULAR,
        ],
        compiler_params=pltpu.CompilerParams(
            collective_id=0,
            has_side_effects=True,
            vmem_limit_bytes=(n_blk + 3 * n_pos) * 2 * JD * hid * cols + 16 * 2**20,
        ),
    )(*[pltpu.with_memory_space_constraint(x, pltpu.HBM) for x in operands])
    return jnp.transpose(result, (1, 0, 2))


def solution(mesh):
    in_specs = (P("blk", "chan", None),) + (P(),) * 11
    out_specs = P("blk", "chan", None)
    return jax.shard_map(
        on_device, mesh=mesh, in_specs=in_specs, out_specs=out_specs, check_vma=False
    )
```

```python
import functools

import jax
import jax.numpy as jnp
from jax import lax
from jax.experimental import pallas as pl
from jax.experimental.pallas import tpu as pltpu
from jax.sharding import PartitionSpec as P

JD = 13
PAD = 16
CHUNKS = 4
HOLD = 1
EPS = 1e-05
F32 = jnp.float32
BF16 = jnp.bfloat16
NT = (((1,), (1,)), ((), ()))
TN = (((0,), (0,)), ((), ()))
NN = (((1,), (0,)), ((), ()))


def xor(a, b, n):
    total, bit = 0, 1
    while bit < n:
        total = total + bit * ((a // bit + b // bit) % 2)
        bit *= 2
    return total


def reverse_bits(t, n):
    total, bit = 0, 1
    while bit < n:
        total = total + (n // 2 // bit) * ((t // bit) % 2)
        bit *= 2
    return total


def sigmoid(x):
    return 0.5 * jnp.tanh(0.5 * x) + 0.5


def layer_norm(x, gain, bias):
    centre = jnp.mean(x, axis=-1, keepdims=True)
    centred = x - centre
    spread = jnp.mean(centred * centred, axis=-1, keepdims=True)
    return centred * lax.rsqrt(spread + EPS) * gain + bias


def gray(t, n):
    return xor(t, t // 2, n)


GROUPS = ((0, 5), (5, 5), (10, 3))


def kernel(
    n_pos,
    slot_size,
    lens_hbm,
    pair_hbm,
    gain_hbm,
    bias_hbm,
    lgate_hbm,
    lvalue_hbm,
    rgate_hbm,
    rvalue_hbm,
    ogain_hbm,
    obias_hbm,
    oweight_hbm,
    gweight_hbm,
    out,
    lens,
    vectors,
    raw,
    pair,
    weights,
    right_all,
    left,
    r0,
    r1,
    work,
    send,
    own,
    recv,
    relay,
    gate_in,
    gate_val,
    load_sem,
    sent,
    rs_recv,
    fw_recv,
    ps_recv,
    rl_recv,
    ready,
):
    rows, cols, ch = pair.shape
    hid = raw.shape[2]
    part = hid // CHUNKS
    pitch = 2 * rows + 8
    total = n_pos * CHUNKS
    last = n_pos - 1
    half = n_pos // 2
    blk = lax.axis_index("blk")
    z = lax.axis_index("chan")
    q = blk // 2
    h = blk % 2
    partner = 2 * q + 1 - h

    def load(n, src, dst):
        copy = pltpu.make_async_copy(src, dst, load_sem.at[n])
        copy.start()
        return copy

    first = [
        load(0, pair_hbm.at[pl.ds(0, JD)], pair.at[pl.ds(0, JD)]),
        load(1, rgate_hbm, raw.at[0]),
        load(2, rvalue_hbm, raw.at[1]),
        load(3, gain_hbm, vectors.at[pl.ds(0, 1)]),
        load(4, bias_hbm, vectors.at[pl.ds(8, 1)]),
        load(5, lens_hbm, lens),
    ]
    def relayed(source, p):
        return ((source == 0) & (p >= half)) | ((source == last) & (p < half))

    def across(source, p):
        return ((source == 1) & (p == last)) | ((source == last - 1) & (p == 0))

    next_in = jnp.where(z == 0, 1, jnp.where(z == last, last - 1, -1))
    behind = jnp.where(z == 1, 0, jnp.where(z == last - 1, last, -1))

    fed = behind >= 0
    barrier = pltpu.get_barrier_semaphore()
    for d in range(1, n_pos):
        pl.semaphore_signal(barrier, inc=1, device_id={"blk": 2 * xor(q, d, n_pos) + h})
        source = xor(z, d, n_pos)

        @pl.when(jnp.logical_not(relayed(source, z) | across(source, z)))
        def _():
            pl.semaphore_signal(barrier, inc=1, device_id={"chan": source})

    pl.semaphore_signal(barrier, inc=1, device_id={"blk": partner})

    def turn(n):
        weights[n * hid : (n + 1) * hid, :] = (0.5 * raw[n].astype(F32)).T.astype(BF16)

    for copy in first:
        copy.wait()
    second = [
        load(6, pair_hbm.at[pl.ds(JD, rows - JD)], pair.at[pl.ds(JD, rows - JD)]),
        load(7, lgate_hbm, raw.at[2]),
        load(8, lvalue_hbm, raw.at[3]),
    ]
    third = [
        load(9, gweight_hbm, raw.at[4]),
        load(10, oweight_hbm, raw.at[5]),
        load(11, ogain_hbm, vectors.at[pl.ds(16, 1)]),
        load(12, obias_hbm, vectors.at[pl.ds(24, 1)]),
    ]
    turn(0)
    turn(1)

    col = z * cols + lax.broadcasted_iota(jnp.int32, (1, cols), 1)
    chain = col // slot_size
    chain_len = jnp.zeros_like(col)
    for s in range(lens.shape[0]):
        chain_len = jnp.where(chain == s, lens[s], chain_len)
    col_real = (col % slot_size < chain_len).astype(F32)

    def row_real(i):
        pos = blk * rows + i
        return jnp.where(pos % slot_size < lens[pos // slot_size], 1.0, 0.0).astype(F32)

    gain_v, bias_v = vectors[0:1, :] * ch**0.5, vectors[8:9, :]
    average = jnp.full((ch, ch), 1.0 / ch, BF16)

    def norm_rows(i, count, by_matmul):
        x = pair[pl.ds(i, count)].reshape(count * cols, ch)
        if by_matmul:
            centre = lax.dot_general(x, average, NN, preferred_element_type=F32)
        else:
            centre = jnp.mean(x.astype(F32), axis=-1, keepdims=True)
        centred = x.astype(F32) - centre
        spread = jnp.sum(centred * centred, axis=-1, keepdims=True)
        return (centred * lax.rsqrt(spread + ch * EPS) * gain_v + bias_v).astype(BF16)

    normed = norm_rows(0, JD, True)
    mix = lax.dot_general(weights[: 2 * hid, :], normed, NT, preferred_element_type=F32)
    val = (jnp.tanh(mix[:hid]) + 1.0) * mix[hid:]
    for m in range(JD):
        row = (val[:, m * cols : (m + 1) * cols] * (col_real * row_real(m))).astype(BF16)
        for k in range(CHUNKS):
            right_all[blk, k, m * part : (m + 1) * part, :] = row[k * part : (k + 1) * part]

    direct = jnp.where(next_in >= 0, half - 1, jnp.where(fed, last - 1, last))
    pl.semaphore_wait(barrier, direct + n_pos)

    @pl.when(fed)
    def _():
        pl.semaphore_signal(ready, inc=1, device_id={"chan": last - z})


    def right_copy(d, k):
        return pltpu.make_async_remote_copy(
            src_ref=right_all.at[blk, k],
            dst_ref=right_all.at[blk, k],
            send_sem=sent.at[0],
            recv_sem=rs_recv.at[d, k],
            device_id={"blk": 2 * xor(q, d, n_pos) + h},
        )

    def forward_copy(d, k):
        mine = 2 * xor(q, d, n_pos) + h
        return pltpu.make_async_remote_copy(
            src_ref=right_all.at[mine, k],
            dst_ref=right_all.at[mine, k],
            send_sem=sent.at[1],
            recv_sem=fw_recv.at[d, k],
            device_id={"blk": partner},
        )

    hops = sorted(range(1, n_pos), key=int.bit_count)
    close = n_pos.bit_length() - 1
    for d in hops[:close]:
        right_copy(d, 0).start()
    forward_copy(0, 0).start()

    def send_rest():
        for k in range(CHUNKS):
            for d in hops[close if k == 0 else 0 :]:
                right_copy(d, k).start()
            if k > 0:
                forward_copy(0, k).start()

    for copy in second:
        copy.wait()
    turn(2)
    turn(3)

    def left_rows(t, carry):
        i = 16 * t
        normed = norm_rows(i, 16, True)
        for u in range(16):
            for g in range(2):
                gate_in[pl.ds(g * rows + i + u, JD, stride=pitch), :] = normed[
                    u * cols + g * rows : u * cols + g * rows + JD
                ].astype(F32)
        mix = lax.dot_general(weights[2 * hid :, :], normed, NT, preferred_element_type=F32)
        val = (jnp.tanh(mix[:hid]) + 1.0) * mix[hid:]
        for u in range(16):
            left[pl.ds(i + u, hid, stride=rows + 8), :] = val[:, u * cols : (u + 1) * cols] * (
                col_real * row_real(i + u)
            )

        @pl.when(t == HOLD)
        def _():
            send_rest()

        return carry

    lax.fori_loop(0, rows // 16, left_rows, 0)

    @pl.when(fed)
    def _():
        pl.semaphore_wait(ready, 1)

    def partial_copy(p, k):
        e = xor(z, p, n_pos)
        return pltpu.make_async_remote_copy(
            src_ref=send.at[p, k],
            dst_ref=recv.at[e, k],
            send_sem=sent.at[2],
            recv_sem=ps_recv.at[jnp.where(e == 1, n_pos + k, e)],
            device_id={"chan": p},
        )

    def group_copy(p, n):
        start, count = GROUPS[n]
        here = pl.ds(start * part, count * part)
        return pltpu.make_async_remote_copy(
            src_ref=send.at[p, pl.ds(1, CHUNKS - 1), here],
            dst_ref=recv.at[1, pl.ds(1, CHUNKS - 1), here],
            send_sem=sent.at[2],
            recv_sem=ps_recv.at[n_pos + 1 + n],
            device_id={"chan": p},
        )

    def relay_copy(p, k):
        return pltpu.make_async_remote_copy(
            src_ref=send.at[p, k],
            dst_ref=relay.at[p, k],
            send_sem=sent.at[2],
            recv_sem=rl_recv.at[p % half, k],
            device_id={"chan": jnp.where(z < half, 1, last - 1)},
        )

    same_side = q // half == z // half

    def side(d):
        return jnp.where(same_side, reverse_bits(d, n_pos), d)

    near, far = side(gray(1, n_pos)), side(gray(last, n_pos))

    def place(s):
        j = s % n_pos
        j = jnp.where((j < 3) & (q == z), (j + 1) % 3, j)
        t = jnp.where(j < 2, j, jnp.where(j == 2, last, j - 1))
        return side(gray(t, n_pos)), s // n_pos

    def pass_on(s, on):
        d, k = place(s)
        p = xor(q, d, n_pos)

        @pl.when(on & relayed(behind, p))
        def _():
            relay_copy(p, k).wait_recv()
            send[p, k] = (send[p, k].astype(F32) + relay[p, k].astype(F32)).astype(BF16)
            partial_copy(p, k).start()

    def share(d, k):
        right_copy(d, k).wait_recv()
        forward_copy(d, k).start()

    def step(s, carry):
        d, k = place(s)
        p = xor(q, d, n_pos)
        opens = s % n_pos == 0

        @pl.when(opens & (q == z))
        def _():
            share(near, k)
            share(far, k)

        @pl.when(s % n_pos > 2)
        def _():
            share(d, k)

        forward_copy(d, k).wait_recv()
        for g, dst in enumerate((r0, r1)):
            for m in range(JD):
                dst[pl.ds(m, part, stride=PAD + 8), :] = right_all[
                    2 * p + g, k, m * part : (m + 1) * part, :
                ].astype(F32)

        base = pl.multiple_of(k * part * (rows + 8), 8)
        for c in range(part):
            rr = slice(c * (PAD + 8), c * (PAD + 8) + PAD)
            lhs = jnp.concatenate([r0[rr, :], r1[rr, :]], axis=0).astype(BF16)
            lc = left[pl.ds(base + c * (rows + 8), rows), :].astype(BF16)
            o = lax.dot_general(lhs, lc, NT, preferred_element_type=F32)
            work[pl.ds(c, PAD, stride=part + 8), :] = jnp.concatenate([o[:PAD], o[PAD:]], axis=1)

        @pl.when(p == z)
        def _():
            for m in range(JD):
                own[k, m * part : (m + 1) * part, :] = work[
                    m * (part + 8) : m * (part + 8) + part, :
                ]

        @pl.when(p != z)
        def _():
            for m in range(JD):
                send[p, k, m * part : (m + 1) * part, :] = work[
                    m * (part + 8) : m * (part + 8) + part, :
                ].astype(BF16)

            @pl.when(relayed(z, p))
            def _():
                relay_copy(p, k).start()

            later = ((p == next_in) & ((k > 0) | jnp.logical_not(same_side))) | relayed(behind, p)

            @pl.when(jnp.logical_not(relayed(z, p) | later))
            def _():
                partial_copy(p, k).start()

        @pl.when(opens & (q != z))
        def _():
            share(near, k)

            @pl.when(k > 0)
            def _():
                share(far, k)

        @pl.when((s == 1) & (q != z))
        def _():
            share(far, 0)

        pass_on(jnp.maximum(s - n_pos, 0), s >= n_pos)
        return carry

    lax.fori_loop(0, total, step, 0)

    @pl.when((next_in >= 0) & jnp.logical_not(same_side))
    def _():
        partial_copy(next_in, 0).start()

    @pl.when(next_in >= 0)
    def _():
        for n in range(len(GROUPS)):
            group_copy(next_in, n).start()

    def rest(j, carry):
        pass_on(total - n_pos + j, True)
        return carry

    lax.fori_loop(0, n_pos, rest, 0)

    for copy in third:
        copy.wait()

    def gates(m, carry):
        mix = lax.dot_general(
            gate_in[pl.ds(pl.multiple_of(m * pitch, 8), 2 * rows), :].astype(BF16),
            raw[4],
            NN,
            preferred_element_type=F32,
        )
        gate_val[m] = sigmoid(mix)
        return carry

    lax.fori_loop(0, JD, gates, 0)

    ogain_v = jnp.broadcast_to(vectors[16:17, :], (2 * rows, hid)).T
    obias_v = jnp.broadcast_to(vectors[24:25, :], (2 * rows, hid)).T
    for e in range(2, n_pos):
        source = xor(z, e, n_pos)

        @pl.when(jnp.logical_not(relayed(source, z)))
        def _():
            pltpu.make_async_remote_copy(
                src_ref=send.at[source],
                dst_ref=recv.at[e],
                send_sem=sent.at[2],
                recv_sem=ps_recv.at[e],
                device_id={"chan": source},
            ).wait_recv()

            def gather(k, carry):
                own[k] = own[k] + recv[e, k].astype(F32)
                return carry

            lax.fori_loop(0, CHUNKS, gather, 0)

    @pl.when(jnp.logical_not(fed))
    def _():
        for k in range(CHUNKS):
            partial_copy(xor(z, 1, n_pos), k).wait_recv()

    def finish(m):
        here = slice(m * part, (m + 1) * part)
        total = jnp.concatenate(
            [own[k, here, :] + recv[1, k, here, :].astype(F32) for k in range(CHUNKS)], axis=0
        )
        total = total.astype(BF16).astype(F32)
        centred = total - jnp.mean(total, axis=0, keepdims=True)
        spread = jnp.mean(centred * centred, axis=0, keepdims=True)
        normed = (centred * lax.rsqrt(spread + EPS) * ogain_v + obias_v).astype(BF16)
        val = lax.dot_general(normed, raw[5], TN, preferred_element_type=F32)
        val = (val * gate_val[m]).astype(BF16)
        for g in range(2):
            out[g * JD + m] = val[g * rows : (g + 1) * rows]

    @pl.when(fed)
    def _():
        partial_copy(behind, 0).wait_recv()

    for n, (start, count) in enumerate(GROUPS):

        @pl.when(fed)
        def _():
            group_copy(behind, n).wait_recv()

        for m in range(start, start + count):
            finish(m)
    def drain(n, blocks, buffer):
        here = buffer.at[pl.ds(0, blocks)]
        pltpu.make_async_remote_copy(
            src_ref=here,
            dst_ref=here,
            send_sem=sent.at[n],
            recv_sem=ps_recv.at[0],
            device_id={"blk": partner},
        ).wait_send()

    drain(0, n_pos - 1, right_all)
    drain(1, n_pos, right_all)
    drain(2, n_pos - 1, send)


def on_device(pair, lengths, gain, bias, lg, lv, rg, rv, ogain, obias, ow, gw):
    rows, cols, ch = pair.shape
    hid = lg.shape[1]
    n_blk = lax.axis_size("blk")
    n_pos = lax.axis_size("chan")
    assert n_blk == 2 * n_pos and cols == 2 * rows and n_pos >= 4 and n_pos & (n_pos - 1) == 0
    slot_size = rows * n_blk // lengths.shape[0]
    part = hid // CHUNKS
    block = (CHUNKS, JD * part, cols)
    operands = (
        lengths,
        pair,
        gain.reshape(1, ch),
        bias.reshape(1, ch),
        lg,
        lv,
        rg,
        rv,
        ogain.reshape(1, hid),
        obias.reshape(1, hid),
        ow,
        gw,
    )
    result = pl.pallas_call(
        functools.partial(kernel, n_pos, slot_size),
        out_shape=jax.ShapeDtypeStruct((2 * JD, rows, ch), BF16),
        in_specs=[pl.BlockSpec(memory_space=pl.ANY)] * 12,
        out_specs=pl.BlockSpec(memory_space=pltpu.VMEM),
        scratch_shapes=[
            pltpu.SMEM(lengths.shape, jnp.int32),
            pltpu.VMEM((32, ch), F32),
            pltpu.VMEM((6, ch, hid), BF16),
            pltpu.VMEM((rows, cols, ch), BF16),
            pltpu.VMEM((4 * hid, ch), BF16),
            pltpu.VMEM((n_blk,) + block, BF16),
            pltpu.VMEM((hid * (rows + 8), cols), F32),
            pltpu.VMEM((part * (PAD + 8), cols), F32),
            pltpu.VMEM((part * (PAD + 8), cols), F32),
            pltpu.VMEM((PAD * (part + 8), 2 * rows), F32),
            pltpu.VMEM((n_pos,) + block, BF16),
            pltpu.VMEM(block, F32),
            pltpu.VMEM((n_pos,) + block, BF16),
            pltpu.VMEM((n_pos,) + block, BF16),
            pltpu.VMEM((PAD * (2 * rows + 8), ch), F32),
            pltpu.VMEM((JD, 2 * rows, ch), F32),
            pltpu.SemaphoreType.DMA((13,)),
            pltpu.SemaphoreType.DMA((3,)),
            pltpu.SemaphoreType.DMA((n_pos, CHUNKS)),
            pltpu.SemaphoreType.DMA((n_pos, CHUNKS)),
            pltpu.SemaphoreType.DMA((n_pos + CHUNKS,)),
            pltpu.SemaphoreType.DMA((n_pos // 2, CHUNKS)),
            pltpu.SemaphoreType.REGULAR,
        ],
        compiler_params=pltpu.CompilerParams(
            collective_id=0,
            has_side_effects=True,
            vmem_limit_bytes=(n_blk + 3 * n_pos) * 2 * JD * hid * cols + 16 * 2**20,
        ),
    )(*[pltpu.with_memory_space_constraint(x, pltpu.HBM) for x in operands])
    return jnp.transpose(result, (1, 0, 2))


def solution(mesh):
    in_specs = (P("blk", "chan", None),) + (P(),) * 11
    out_specs = P("blk", "chan", None)
    return jax.shard_map(
        on_device, mesh=mesh, in_specs=in_specs, out_specs=out_specs, check_vma=False
    )
```
